32 devices in a mesh: gx: 8 (over z, x), gy: 4 (over y, core).
Axes of the slice: x: 2, y: 2, z: 4, core: 2. Of those that a mesh axis runs over, the one named last changes fastest.
Arguments:
- pressure: float32 [256, 128, 128], P('gx', 'gy'), may hold values from -6 to 6
- depth: float32 [256, 128, 128], P('gx', 'gy'), may hold values from -6 to 6
- saturation: float32 [2, 256, 128, 128], P(None, 'gx', 'gy'), may hold values from 0.05 to 0.45
- permeability: float32 [3, 256, 128, 128], P(None, 'gx', 'gy'), may hold values from 0.1 to 10
- pore_volume: float32 [256, 128, 128], P('gx', 'gy'), may hold values from 0.5 to 2
- fault_pairs: int32 [1024, 3], P(('gx', 'gy')), may hold values from 0 to 1023, as said below
- fault_kind: int32 [1024], P(('gx', 'gy')), may hold values from 0 to 15
- fault_count: int32 [32], P(('gx', 'gy')), may hold values from 8 to 32, as said below
- fault_table: float32 [16, 128], replicated, may hold values from 0.2 to 2
Outputs:
- saturation_next: float32 [3, 256, 128, 128], P(None, 'gx', 'gy')
The draws below stay inside these ranges and needn't reach their ends.
Inputs may be any that keep to these rules, and one draw needn't show every extreme that they name: `fault_pairs`: each device holds 32 rows. Column 0 and column 2 are areal column numbers a * 32 + b of the source and target device. Column 1 is the target device i2 * 4 + j2, which lies within one index of the source device along gx and along gy, counted cyclically. Among one device's 32 rows at most 4 name the same target device, and on every device some target device is named by exactly 4 rows. Rows 0 to fault_count - 1 of a device are live; some device has 32 live rows.
All inputs are finite; a program needn't handle non-finite values.
Results may differ from the reference program's by a relative error of at most 0.0003.
Values sent between devices are 32-bit elements; how exact they have to be, the bound alone decides.
A program may use at most 64 MiB of HBM per device.

```python
import math
import jax
import jax.numpy as jnp
from jax import lax

CX = 32
CY = 32
NZ = 128
FB = 32
CAP = 4
NTAB = 16
NX = 256
NY = 128
N_GX = 8
N_GY = 4


def draw_fault_pairs(key, part):
    devices = N_GX * N_GY

    def one_device(device_key, device):
        order = jax.random.permutation(jax.random.fold_in(device_key, 1), 9 * CAP)[:FB].astype(jnp.int32)
        near = order // CAP
        step_x = near // 3 - 1
        step_y = near % 3 - 1
        home_x = device // N_GY
        home_y = device % N_GY
        target = (home_x + step_x) % N_GX * N_GY + (home_y + step_y) % N_GY
        source = jax.random.randint(jax.random.fold_in(device_key, 2), (FB,), 0, CX * CY, dtype=jnp.int32)
        landing = jax.random.randint(jax.random.fold_in(device_key, 3), (FB,), 0, CX * CY, dtype=jnp.int32)
        return jnp.stack([source, target.astype(jnp.int32), landing], axis=1)
    keys = jax.random.split(jax.random.fold_in(key, 11), devices)
    device_ids = jnp.arange(devices, dtype=jnp.int32)
    return jax.vmap(one_device)(keys, device_ids).reshape(devices * FB, 3)


def draw_fault_count(key, part):
    devices = N_GX * N_GY
    levels = jax.random.randint(jax.random.fold_in(key, 21), (devices,), 0, 3, dtype=jnp.int32)
    counts = jnp.where(levels == 0, FB, jnp.where(levels == 1, FB // 2, FB // 4)).astype(jnp.int32)
    busiest = jax.random.randint(jax.random.fold_in(key, 22), (), 0, devices, dtype=jnp.int32)
    return jnp.where(jnp.arange(devices, dtype=jnp.int32) == busiest, FB, counts).astype(jnp.int32)


def set_ends(entries, own_key, low, largest):
    index_at = [jax.random.randint(jax.random.fold_in(own_key, axis), (), 0, length) for axis, length in enumerate(entries.shape)]
    widest = entries.shape.index(max(entries.shape))
    beside = index_at[:widest] + [(index_at[widest] + 1) % entries.shape[widest]] + index_at[widest + 1:]
    return entries.at[tuple(index_at)].set(low).at[tuple(beside)].set(largest)


def shard_levels(key, dims, cuts, smallest, top_value):
    loudness, own = 1.0, jax.random.fold_in(key, 6)
    for dim, parts in cuts:
        draws = jnp.exp(jax.random.uniform(jax.random.fold_in(own, dim), (parts,), jnp.float32, smallest / len(cuts), top_value / len(cuts)))
        loudness = loudness * jnp.repeat(draws, dims[dim] // parts).reshape([-1 if axis == dim else 1 for axis in range(len(dims))])
    return loudness


def normal_values(own_key, dims, spread, reach, cuts=(), held_as=jnp.bfloat16):
    factor_of = shard_levels(own_key, dims, cuts, -0.22, 0.18) if cuts else 1.0
    values = jax.random.normal(own_key, dims, jnp.float32) * spread * factor_of
    return jnp.minimum(jnp.maximum(values, -reach), reach).astype(held_as)


def setup_inputs(seed: int = 0) -> dict:
    streams_of = jax.random.split(jax.random.key(seed), 10)
    pressure = normal_values(streams_of[0], (NX, NY, NZ), 1.0, 6.0, ((0, 8), (1, 4)), jnp.float32)
    depth = normal_values(streams_of[1], (NX, NY, NZ), 1.0, 6.0, ((0, 8), (1, 4)), jnp.float32)
    saturation = jnp.clip(0.05 + 0.39999999 * jax.random.uniform(streams_of[2], (2, NX, NY, NZ), jnp.float32) ** shard_levels(streams_of[2], (2, NX, NY, NZ), ((1, 8), (2, 4)), -0.2, 0.2), 0.05, 0.45)
    permeability = jnp.clip(jnp.exp(math.log(10.0) - 4.6051702 * jax.random.uniform(streams_of[3], (3, NX, NY, NZ), jnp.float32) ** shard_levels(streams_of[3], (3, NX, NY, NZ), ((1, 8), (2, 4)), -0.2, 0.2)), 0.1, 10.0)
    pore_volume = jnp.clip(jnp.exp(math.log(2.0) - 1.3862944 * jax.random.uniform(streams_of[4], (NX, NY, NZ), jnp.float32) ** shard_levels(streams_of[4], (NX, NY, NZ), ((0, 8), (1, 4)), -0.2, 0.2)), 0.5, 2.0)
    fault_pairs = draw_fault_pairs(jax.random.fold_in(streams_of[9], 71), 0)
    fault_kind = set_ends(jax.random.randint(streams_of[6], (N_GX * N_GY * FB,), 0, NTAB), jax.random.fold_in(streams_of[6], 1), 0, NTAB - 1).astype(jnp.int32)
    fault_count = draw_fault_count(jax.random.fold_in(streams_of[9], 71), 0)
    fault_table = jnp.clip(jnp.exp(jax.random.uniform(streams_of[8], (NTAB, NZ), jnp.float32, math.log(0.2), math.log(2.0))), 0.2, 2.0)
    return dict(pressure=pressure, depth=depth, saturation=saturation, permeability=permeability, pore_volume=pore_volume, fault_pairs=fault_pairs, fault_kind=fault_kind, fault_count=fault_count, fault_table=fault_table)


VISCOSITY = (0.5, 1.0, 0.25)
DENSITY = (1.0, 0.8, 0.25)
step_length = 0.2


def mobility(sat_water, sat_oil):
    sat_gas = 1.0 - sat_water - sat_oil
    return (sat_water * sat_water / VISCOSITY[0], sat_oil * sat_oil / VISCOSITY[1], sat_gas * sat_gas / VISCOSITY[2])


def harmonic(first, second):
    return 2.0 * first * second / (first + second)


def phase_flux(press_low, depth_low, mobile_low, press_high, depth_high, mobile_high, trans):
    flows = []
    for phase in range(3):
        drive = (press_low - press_high) - DENSITY[phase] * (depth_low - depth_high)
        upwind = jnp.where(drive > 0.0, mobile_low[phase], mobile_high[phase])
        flows.append(trans * upwind * drive)
    return jnp.stack(flows, axis=-2)


def consecutive(array, axis, start):
    return lax.slice_in_dim(array, start, array.shape[axis] - 1 + start, axis=axis)


def face_flows(press, height, mobile, perm, axis):
    def lower(array):
        return consecutive(array, axis, 0)

    def upper(array):
        return consecutive(array, axis, 1)

    return phase_flux(lower(press), lower(height), tuple(lower(m) for m in mobile),
                      upper(press), upper(height), tuple(upper(m) for m in mobile),
                      harmonic(lower(perm), upper(perm)))


def reference(pressure, depth, saturation, permeability, pore_volume, fault_pairs, fault_kind, fault_count, fault_table):
    sat_water = saturation[0]
    sat_oil = saturation[1]
    mobile = mobility(sat_water, sat_oil)
    flow_x = jnp.pad(face_flows(pressure, depth, mobile, permeability[0], 0), ((1, 1), (0, 0), (0, 0), (0, 0)))
    flow_y = jnp.pad(face_flows(pressure, depth, mobile, permeability[1], 1), ((0, 0), (1, 1), (0, 0), (0, 0)))
    flow_z = jnp.pad(face_flows(pressure, depth, mobile, permeability[2], 2), ((0, 0), (0, 0), (0, 0), (1, 1)))
    net = (flow_x[1:] - flow_x[:-1]) + (flow_y[:, 1:] - flow_y[:, :-1]) + (flow_z[..., 1:] - flow_z[..., :-1])
    devices = N_GX * N_GY
    pairs = fault_pairs.reshape(devices, FB, 3)
    device = jnp.arange(devices, dtype=jnp.int32)[:, None]
    home_x = device // N_GY
    home_y = device % N_GY
    source = ((home_x * CX + pairs[..., 0] // CY) * NY + home_y * CY + pairs[..., 0] % CY).reshape(-1)
    target = pairs[..., 1]
    dest = (((target // N_GY) * CX + pairs[..., 2] // CY) * NY + (target % N_GY) * CY + pairs[..., 2] % CY).reshape(-1)
    live = (jnp.arange(FB, dtype=jnp.int32)[None, :] < fault_count[:, None]).reshape(-1)
    trans = fault_table[fault_kind] * live[:, None].astype(jnp.float32)
    press_flat = pressure.reshape(NX * NY, NZ)
    depth_flat = depth.reshape(NX * NY, NZ)
    mobile_flat = tuple(m.reshape(NX * NY, NZ) for m in mobile)
    fault_flow = phase_flux(press_flat[source], depth_flat[source], tuple(m[source] for m in mobile_flat),
                            press_flat[dest], depth_flat[dest], tuple(m[dest] for m in mobile_flat), trans)
    net_flat = net.reshape(NX * NY, 3, NZ).at[source].add(fault_flow).at[dest].add(-fault_flow)
    net = net_flat.reshape(NX, NY, 3, NZ)
    sat_gas = 1.0 - sat_water - sat_oil
    return jnp.stack([current - step_length * net[:, :, phase, :] / pore_volume
                      for phase, current in enumerate((sat_water, sat_oil, sat_gas))], axis=0)
```

```python
import functools

import jax
import jax.numpy as jnp
from jax import lax
from jax.experimental import pallas as pl
from jax.experimental.pallas import tpu as pltpu
from jax.sharding import PartitionSpec as P

CAP = 4
ROWS = 2 * CAP
VISCOSITY = (0.5, 1.0, 0.25)
DENSITY = (1.0, 0.8, 0.25)
STEP = 0.2
MESH = pl.DeviceIdType.MESH
NEAR = [(dx, dy) for dx in (-1, 0, 1) for dy in (-1, 0, 1)]
HOME = 4
OTHERS = [n for n in range(9) if n != HOME]
PIECES = 12


def mobility(w, o):
    g = 1.0 - w - o
    return (w * w * (1.0 / VISCOSITY[0]), o * o, g * g * (1.0 / VISCOSITY[2]))


def harmonic(a, b):
    return 2.0 * a * b / (a + b)


def flux(dp, dd, low, high, trans):
    flows = []
    for f in range(3):
        drive = dp - DENSITY[f] * dd if DENSITY[f] != 1.0 else dp - dd
        flows.append(trans * jnp.where(drive > 0.0, low[f], high[f]) * drive)
    return flows


def edge_flux(low, high):
    return flux(
        low[0] - high[0],
        low[1] - high[1],
        mobility(low[2], low[3]),
        mobility(high[2], high[3]),
        harmonic(low[4], high[4]),
    )


def kernel(
    cx, cy, nz, nrow,
    p_hbm, d_hbm, s_hbm, k_hbm, v_hbm, pairs_hbm, kind_hbm, count_hbm, table_hbm,
    out, res, own_s,
    cell, k, v, table, pairs_v, count_s, kindrow,
    idx_send, idx_s, send, recv, loc, tloc, back, ret, scl,
    xhalo, yhalo,
    load_sem, own_sem, is_sem, ir_sem, fs_sem, fr_sem, bs_sem, br_sem,
    xs_sem, xr_sem, ys_sem, yr_sem,
):
    nx = lax.axis_size("gx")
    ny = lax.axis_size("gy")
    ix = lax.axis_index("gx")
    iy = lax.axis_index("gy")
    cells = cx * cy
    p, d, s = (cell.at[pl.ds(i * cells, (1, 1, 2)[i] * cells)] for i in range(3))

    def device(dx, dy):
        return (lax.rem(ix + dx + nx, nx), lax.rem(iy + dy + ny, ny))

    def remote(src, dst, ss, rs, dev):
        return pltpu.make_async_remote_copy(
            src_ref=src, dst_ref=dst, send_sem=ss, recv_sem=rs, device_id=dev, device_id_type=MESH
        )

    def arrived(ref, sem):
        pltpu.make_async_copy(ref, ref, sem).wait()

    barrier = pltpu.get_barrier_semaphore()
    for n in OTHERS:
        pl.semaphore_signal(barrier, inc=1, device_id=device(*NEAR[n]), device_id_type=MESH)
    loads = [
        pltpu.make_async_copy(src, dst, load_sem.at[i])
        for i, src, dst in (
            (0, pairs_hbm, pairs_v),
            (1, kind_hbm, kindrow),
            (2, count_hbm, count_s),
            (3, p_hbm, p),
            (3, d_hbm, d),
            (3, s_hbm, s),
            (4, k_hbm, k),
            (5, v_hbm, v),
            (6, table_hbm, table),
        )
    ]
    for c in loads:
        c.start()

    for c in loads[:3]:
        c.wait()
    lane_of_row = lax.broadcasted_iota(jnp.int32, (nrow, nrow), 1)
    sub_of_row = lax.broadcasted_iota(jnp.int32, (nrow, nrow), 0)
    eye = lane_of_row == sub_of_row
    pv = pairs_v[...]
    tgt_row = pv[1:2, :]

    def to_sublanes(row):
        return jnp.sum(jnp.where(eye, row, 0), axis=1, keepdims=True)

    src_col = to_sublanes(pv[0:1, :])
    tgt_col = to_sublanes(tgt_row)
    land_col = to_sublanes(pv[2:3, :])
    kind_col = to_sublanes(kindrow[...].reshape(1, nrow))
    rank_col = jnp.sum(
        ((tgt_col == tgt_row) & (lane_of_row < sub_of_row)).astype(jnp.int32), axis=1, keepdims=True
    )
    live_col = (lax.broadcasted_iota(jnp.int32, (nrow, 1), 0) < count_s[0]).astype(jnp.int32)
    code_col = jnp.zeros_like(tgt_col)
    for n in range(9):
        hx, hy = device(*NEAR[n])
        code_col = jnp.where(tgt_col == hx * ny + hy, n, code_col)
    lanes = lax.broadcasted_iota(jnp.int32, (nrow, 128), 1)
    message = (
        jnp.where(lanes == rank_col, land_col, 0)
        + jnp.where(lanes == CAP + rank_col, kind_col, 0)
        + jnp.where(lanes == 2 * CAP + rank_col, live_col, 0)
        + jnp.where(lanes == 3 * CAP + rank_col, src_col, 0)
    )
    for n in range(9):
        idx_send[n] = jnp.sum(jnp.where(code_col == n, message, 0), axis=0, keepdims=True)

    own_copy = pltpu.make_async_copy(idx_send, own_s, own_sem)
    own_copy.start()
    arrived(cell, load_sem.at[3])
    own_copy.wait()
    for n in range(9):
        dst = recv if n == HOME else send
        for r in range(CAP):
            col = own_s[n, 0, 3 * CAP + r]
            dst[n, r : r + 1, :nz] = p[pl.ds(col, 1), :]
            dst[n, CAP + r : CAP + r + 1, :nz] = d[pl.ds(col, 1), :]
            dst[n, r : r + 1, nz:] = s[pl.ds(col, 1), :]
            dst[n, CAP + r : CAP + r + 1, nz:] = s[pl.ds(cells + col, 1), :]

    odd = lax.rem(ix, 2)
    away = 2 * odd - 1

    def ask(dx, dy):
        n = 3 * (dx + 1) + dy + 1
        dev = device(dx, dy)
        remote(idx_send.at[n], idx_s.at[n], is_sem, ir_sem.at[dx + 1], dev).start()
        remote(send.at[n], recv.at[n], fs_sem, fr_sem.at[dx + 1], dev).start()

    pl.semaphore_wait(barrier, 8)
    for dx in (away, -away):
        for dy in (-1, 1, 0):
            ask(dx, dy)
    for dy in (-1, 1):
        ask(0, dy)

    for c in loads[6:]:
        c.wait()
    xparts = [(p, 0), (d, 0), (s, 0), (s, cells), (k, 0)]
    yparts = [(p, 0), (d, 0), (s, 0), (s, cx), (k, cx)]

    def xcopy(side, f):
        ref, base = xparts[f]
        at = base + (0 if side == 0 else cells - cy)
        return remote(
            ref.at[pl.ds(at, cy), :], xhalo.at[1 - side, f], xs_sem.at[side], xr_sem.at[1 - side],
            device(-1 if side == 0 else 1, 0),
        )

    for f in range(5):
        ref, base = yparts[f]
        base = base * cy if f >= 3 else base
        for side in range(2):
            off = base + (0 if side == 0 else cy - 1)
            yhalo[2 + side, f] = ref[pl.ds(off, cx, stride=cy), :]

    def ycopy(side):
        return remote(
            yhalo.at[2 + side], yhalo.at[1 - side], ys_sem.at[side], yr_sem.at[1 - side],
            device(0, -1 if side == 0 else 1),
        )

    has = ((ix > 0, ix < nx - 1), (iy > 0, iy < ny - 1))
    for side in range(2):
        @pl.when(has[0][side])
        def _():
            for f in range(5):
                xcopy(side, f).start()

        @pl.when(has[1][side])
        def _():
            ycopy(side).start()

    zmask = lax.broadcasted_iota(jnp.int32, (cy, nz), 1) < nz - 1
    ymask = lax.broadcasted_iota(jnp.int32, (cy, nz), 0) < cy - 1

    def slab(a, carry):
        base = pl.multiple_of(a * cy, cy)
        after = pl.multiple_of(jnp.minimum(a + 1, cx - 1) * cy, cy)

        def at(ref, off):
            return ref[pl.ds(off, cy), :]

        p0, d0 = at(p, base), at(d, base)
        w0, o0 = at(s, base), at(s, cells + base)
        m0 = mobility(w0, o0)
        m1 = mobility(at(s, after), at(s, cells + after))
        tx = jnp.where(a < cx - 1, harmonic(at(k, base), at(k, after)), 0.0)
        fx = flux(p0 - at(p, after), d0 - at(d, after), m0, m1, tx)
        net = [fx[f] - carry[f] for f in range(3)]
        for axis, size, mask, offset in ((0, cy, ymask, cells), (1, nz, zmask, 2 * cells)):
            def up(x):
                return pltpu.roll(x, size - 1, axis)

            kk = at(k, offset + base)
            t = jnp.where(mask, harmonic(kk, up(kk)), 0.0)
            fl = flux(p0 - up(p0), d0 - up(d0), m0, [up(m) for m in m0], t)
            net = [net[f] + (fl[f] - pltpu.roll(fl[f], 1, axis)) for f in range(3)]
        scale = STEP / at(v, base)
        v[pl.ds(base, cy), :] = scale
        now = (w0, o0, 1.0 - w0 - o0)
        for f in range(3):
            out[pl.ds(f * cells + base, cy), :] = now[f] - scale * net[f]
        return tuple(fx)

    zero = jnp.zeros((cy, nz), jnp.float32)
    lax.fori_loop(0, cx, slab, (zero, zero, zero), unroll=2)

    def answer(group, sources):
        first = 3 * group
        for i, ints in enumerate(sources):
            n = first + i
            for r in range(CAP):
                land = ints[n, 0, r]
                kd = ints[n, 0, CAP + r]
                live = ints[n, 0, 2 * CAP + r].astype(jnp.float32)
                loc[n, r : r + 1, :nz] = p[pl.ds(land, 1), :]
                loc[n, CAP + r : CAP + r + 1, :nz] = d[pl.ds(land, 1), :]
                loc[n, r : r + 1, nz:] = s[pl.ds(land, 1), :]
                loc[n, CAP + r : CAP + r + 1, nz:] = s[pl.ds(cells + land, 1), :]
                tloc[n, r : r + 1, :] = table[pl.ds(kd, 1), :] * live

    def flows_of(group):
        rows = pl.ds(3 * group, 3)
        far, here = recv[rows], loc[rows]

        def second(x):
            return pltpu.roll(x, CAP, 1)

        gap = far[:, :, :nz] - here[:, :, :nz]
        fl = flux(
            gap,
            second(gap),
            mobility(far[:, :, nz:], second(far[:, :, nz:])),
            mobility(here[:, :, nz:], second(here[:, :, nz:])),
            tloc[rows],
        )
        for f in range(3):
            back[rows, :, f * nz : (f + 1) * nz] = fl[f][:, :CAP]

    def reply(dx, dy):
        n = 3 * (dx + 1) + dy + 1
        return remote(back.at[n], ret.at[n], bs_sem, br_sem, device(-dx, -dy))

    for dx in (0, away, -away):
        group = dx + 1
        still = isinstance(dx, int)
        many = 2 if still else 3
        arrived(idx_s.at[pl.ds(3 * group, many)], ir_sem.at[group])
        answer(group, (idx_s, own_s, idx_s) if still else (idx_s,) * 3)
        arrived(recv.at[pl.ds(3 * group, many)], fr_sem.at[group])
        flows_of(group)
        for dy in (-1, 1) if still else (-1, 1, 0):
            reply(dx, dy).start()

    for side in range(2):
        @pl.when(has[0][side])
        def _():
            arrived(xhalo.at[side], xs_sem.at[side])
            arrived(xhalo.at[side], xr_sem.at[side])
            at = 0 if side == 0 else cells - cy
            mine = [ref[pl.ds(base + at, cy), :] for ref, base in xparts]
            near = [xhalo[side, f] for f in range(5)]
            low, high = (near, mine) if side == 0 else (mine, near)
            fl = edge_flux(low, high)
            scale = v[pl.ds(at, cy), :]
            for f in range(3):
                rows = pl.ds(f * cells + at, cy)
                out[rows, :] = out[rows, :] + (scale * fl[f] if side == 0 else -scale * fl[f])

    for side in range(2):
        @pl.when(has[1][side])
        def _():
            ycopy(side).wait_send()
            ycopy(1 - side).wait_recv()
            at = 0 if side == 0 else cy - 1
            mine = [yhalo[2 + side, f] for f in range(5)]
            near = [yhalo[side, f] for f in range(5)]
            low, high = (near, mine) if side == 0 else (mine, near)
            fl = edge_flux(low, high)
            scale = v[pl.ds(at, cx, stride=cy), :]
            for f in range(3):
                rows = pl.ds(f * cells + at, cx, stride=cy)
                out[rows, :] = out[rows, :] + (scale * fl[f] if side == 0 else -scale * fl[f])

    lane1 = lax.broadcasted_iota(jnp.int32, (1, 128), 1)
    slots = 10 * CAP
    spot = jnp.full((1, 128), -1, jnp.int32)
    for n in range(9):
        for r in range(CAP):
            spot = jnp.where(lane1 == n * CAP + r, (own_s if n == HOME else idx_s)[n, 0, r], spot)
    for r in range(CAP):
        spot = jnp.where(lane1 == 9 * CAP + r, own_s[HOME, 0, 3 * CAP + r], spot)
    spot = jnp.where(lane1 < slots, spot, 0)
    spot = spot + pltpu.roll(spot, slots, 1) + pltpu.roll(spot, 2 * slots, 1)
    flows = jnp.concatenate([-back[n] for n in range(9)] + [back[HOME]], axis=0)
    hi = flows.astype(jnp.bfloat16).astype(jnp.float32)
    rest = flows - hi
    mid = rest.astype(jnp.bfloat16).astype(jnp.float32)
    pad = jnp.zeros((128 - 3 * slots, 3 * nz), jnp.float32)
    parts = jnp.concatenate([hi, mid, rest - mid, pad], axis=0).astype(jnp.bfloat16)
    step = 8 * cy
    for c in range(cells // step):
        ids = lax.broadcasted_iota(jnp.int32, (step, 128), 0) + c * step
        hot = (ids == spot).astype(jnp.float32).astype(jnp.bfloat16)
        add = jnp.dot(hot, parts, preferred_element_type=jnp.float32)
        scale = v[c * step : (c + 1) * step, :]
        for f in range(3):
            at = pl.ds(f * cells + c * step, step)
            out[at, :] = out[at, :] - scale * add[:, f * nz : (f + 1) * nz]

    for n in OTHERS:
        for r in range(CAP):
            scl[n, r : r + 1, :] = v[pl.ds(own_s[n, 0, 3 * CAP + r], 1), :]
    arrived(idx_send.at[pl.ds(0, 8)], is_sem)
    arrived(send.at[pl.ds(0, 8)], fs_sem)
    arrived(back.at[pl.ds(0, 8)], bs_sem)
    arrived(ret.at[pl.ds(0, 8)], br_sem)
    for n in OTHERS:
        for f in range(3):
            res[n, :, f * nz : (f + 1) * nz] = ret[n, :, f * nz : (f + 1) * nz] * scl[n]


def finish(cells, nz, part, res_in, own_s, held, res, final, sem):
    for n in OTHERS:
        for r in range(CAP):
            col = own_s[n, 0, 3 * CAP + r]
            for f in range(3):
                row = pl.ds(f * cells + col, 1)
                held[row, :] = held[row, :] - res[n, r : r + 1, f * nz : (f + 1) * nz]
    size = 3 * cells // PIECES
    for i in range(PIECES):
        rows = pl.ds(i * size, size)
        pltpu.make_async_copy(held.at[rows], final.at[rows], sem).start()
    pltpu.make_async_copy(held, final, sem).wait()


def body(pressure, depth, saturation, permeability, pore_volume, pairs, kind, count, table):
    cx, cy, nz = pressure.shape
    nrow = pairs.shape[0]
    kinds = table.shape[0]
    cells = cx * cy
    f32 = jnp.float32
    dma = pltpu.SemaphoreType.DMA
    any_spec = pl.BlockSpec(memory_space=pltpu.HBM)
    vmem = pl.BlockSpec(memory_space=pltpu.VMEM)
    smem = pl.BlockSpec(memory_space=pltpu.SMEM)
    part, res, own = pl.pallas_call(
        functools.partial(kernel, cx, cy, nz, nrow),
        out_shape=(
            pltpu.VMEM((3 * cells, nz), f32),
            pltpu.VMEM((9, CAP, 3 * nz), f32),
            pltpu.SMEM((9, 1, 128), jnp.int32),
        ),
        in_specs=[any_spec] * 9,
        out_specs=(vmem, vmem, smem),
        scratch_shapes=[
            pltpu.VMEM((4 * cells, nz), f32),
            pltpu.VMEM((3 * cells, nz), f32),
            pltpu.VMEM((cells, nz), f32),
            pltpu.VMEM((kinds, nz), f32),
            pltpu.VMEM((3, nrow), jnp.int32),
            pltpu.SMEM((1,), jnp.int32),
            pltpu.VMEM((nrow,), jnp.int32),
            pltpu.VMEM((9, 1, 128), jnp.int32),
            pltpu.SMEM((9, 1, 128), jnp.int32),
            pltpu.VMEM((9, ROWS, 2 * nz), f32),
            pltpu.VMEM((9, ROWS, 2 * nz), f32),
            pltpu.VMEM((9, ROWS, 2 * nz), f32),
            pltpu.VMEM((9, ROWS, nz), f32),
            pltpu.VMEM((9, CAP, 3 * nz), f32),
            pltpu.VMEM((9, CAP, 3 * nz), f32),
            pltpu.VMEM((9, CAP, nz), f32),
            pltpu.VMEM((2, 5, cy, nz), f32),
            pltpu.VMEM((4, 5, cx, nz), f32),
            dma((7,)), dma,
            dma, dma((3,)), dma, dma((3,)), dma, dma,
            dma((2,)), dma((2,)), dma((2,)), dma((2,)),
        ],
        compiler_params=pltpu.CompilerParams(
            collective_id=0, has_side_effects=True, vmem_limit_bytes=60000000
        ),
    )(
        pressure.reshape(cells, nz),
        depth.reshape(cells, nz),
        saturation.reshape(2 * cells, nz),
        permeability.reshape(3 * cells, nz),
        pore_volume.reshape(cells, nz),
        pairs.T,
        kind,
        count,
        table,
    )
    _, _, out = pl.pallas_call(
        functools.partial(finish, cells, nz),
        out_shape=(
            pltpu.VMEM((3 * cells, nz), f32),
            pltpu.VMEM((9, CAP, 3 * nz), f32),
            jax.ShapeDtypeStruct((3 * cells, nz), f32),
        ),
        in_specs=[vmem, vmem, smem],
        out_specs=(vmem, vmem, any_spec),
        scratch_shapes=[dma],
        input_output_aliases={0: 0, 1: 1},
    )(part, res, own)
    return out.reshape(3, cx, cy, nz)


def solution(mesh):
    cell = P("gx", "gy", None)
    cells = P(None, "gx", "gy", None)
    both = ("gx", "gy")
    return jax.shard_map(
        body,
        mesh=mesh,
        in_specs=(cell, cell, cells, cells, cell, P(both, None), P(both), P(both), P()),
        out_specs=cells,
        check_vma=False,
    )
```

```python
import functools

import jax
import jax.numpy as jnp
from jax import lax
from jax.experimental import pallas as pl
from jax.experimental.pallas import tpu as pltpu
from jax.sharding import PartitionSpec as P

CAP = 4
ROWS = 2 * CAP
VISCOSITY = (0.5, 1.0, 0.25)
DENSITY = (1.0, 0.8, 0.25)
STEP = 0.2
MESH = pl.DeviceIdType.MESH
NEAR = [(dx, dy) for dx in (-1, 0, 1) for dy in (-1, 0, 1)]
HOME = 4
OTHERS = [n for n in range(9) if n != HOME]
PIECES = 12


def mobility(w, o):
    g = 1.0 - w - o
    return (w * w * (1.0 / VISCOSITY[0]), o * o, g * g * (1.0 / VISCOSITY[2]))


def harmonic(a, b):
    return 2.0 * a * b / (a + b)


def flux(dp, dd, low, high, trans):
    flows = []
    for f in range(3):
        drive = dp - DENSITY[f] * dd if DENSITY[f] != 1.0 else dp - dd
        flows.append(trans * jnp.where(drive > 0.0, low[f], high[f]) * drive)
    return flows


def edge_flux(low, high):
    return flux(
        low[0] - high[0],
        low[1] - high[1],
        mobility(low[2], low[3]),
        mobility(high[2], high[3]),
        harmonic(low[4], high[4]),
    )


def kernel(
    cx, cy, nz, nrow,
    p_hbm, d_hbm, s_hbm, k_hbm, v_hbm, pairs_hbm, kind_hbm, count_hbm, table_hbm,
    out, res, own_s,
    cell, k, v, table, pairs_v, count_s, kindrow,
    idx_send, idx_s, send, recv, loc, tloc, back, ret, scl,
    xhalo, yhalo,
    load_sem, own_sem, is_sem, ir_sem, fs_sem, fr_sem, bs_sem, br_sem,
    xs_sem, xr_sem, ys_sem, yr_sem,
    between, via_i, via_f, vi_sem, vf_sem, ws_sem, go_sem, here_sem,
):
    nx = lax.axis_size("gx")
    ny = lax.axis_size("gy")
    ix = lax.axis_index("gx")
    iy = lax.axis_index("gy")
    cells = cx * cy
    p, d, s = (cell.at[pl.ds(i * cells, (1, 1, 2)[i] * cells)] for i in range(3))

    def device(dx, dy):
        return (lax.rem(ix + dx + nx, nx), lax.rem(iy + dy + ny, ny))

    def remote(src, dst, ss, rs, dev):
        return pltpu.make_async_remote_copy(
            src_ref=src, dst_ref=dst, send_sem=ss, recv_sem=rs, device_id=dev, device_id_type=MESH
        )

    def arrived(ref, sem):
        pltpu.make_async_copy(ref, ref, sem).wait()

    def signal(sem, dev):
        pl.semaphore_signal(sem, inc=1, device_id=dev, device_id_type=MESH)

    def wrap(y):
        return lax.rem(y + 2 * ny, ny)

    first, last = ix == 0, ix == nx - 1
    y_odd = lax.rem(iy, 2)
    relays = (ix == 1) & (y_odd == 1)
    barrier = pltpu.get_barrier_semaphore()
    for n in OTHERS:
        dx, dy = NEAR[n]
        if dx == 1:
            @pl.when(ix < nx - 2)
            def _():
                signal(barrier, device(dx, dy))
        elif dx == 0:
            @pl.when(~last)
            def _():
                signal(barrier, device(dx, dy))
        else:
            signal(barrier, device(dx, dy))

    @pl.when(relays)
    def _():
        signal(barrier, (nx - 1, wrap(iy - 1)))
        signal(barrier, (nx - 1, iy))
        signal(barrier, (0, wrap(iy - 2)))

    loads = [
        pltpu.make_async_copy(src, dst, load_sem.at[i])
        for i, src, dst in (
            (0, pairs_hbm, pairs_v),
            (1, kind_hbm, kindrow),
            (2, count_hbm, count_s),
            (3, p_hbm, p),
            (3, d_hbm, d),
            (3, s_hbm, s),
            (4, k_hbm, k),
            (5, v_hbm, v),
            (6, table_hbm, table),
        )
    ]
    for c in loads:
        c.start()

    @pl.when(last)
    def _():
        pl.semaphore_wait(barrier, 4)
        signal(go_sem.at[y_odd], (1, iy + 1 - y_odd))
        for dy in (-1, 0, 1):
            signal(here_sem, (0, wrap(iy + dy)))

    for c in loads[:3]:
        c.wait()
    lane_of_row = lax.broadcasted_iota(jnp.int32, (nrow, nrow), 1)
    sub_of_row = lax.broadcasted_iota(jnp.int32, (nrow, nrow), 0)
    eye = lane_of_row == sub_of_row
    pv = pairs_v[...]
    tgt_row = pv[1:2, :]

    def to_sublanes(row):
        return jnp.sum(jnp.where(eye, row, 0), axis=1, keepdims=True)

    src_col = to_sublanes(pv[0:1, :])
    tgt_col = to_sublanes(tgt_row)
    land_col = to_sublanes(pv[2:3, :])
    kind_col = to_sublanes(kindrow[...].reshape(1, nrow))
    rank_col = jnp.sum(
        ((tgt_col == tgt_row) & (lane_of_row < sub_of_row)).astype(jnp.int32), axis=1, keepdims=True
    )
    live_col = (lax.broadcasted_iota(jnp.int32, (nrow, 1), 0) < count_s[0]).astype(jnp.int32)
    code_col = jnp.zeros_like(tgt_col)
    for n in range(9):
        hx, hy = device(*NEAR[n])
        code_col = jnp.where(tgt_col == hx * ny + hy, n, code_col)
    lanes = lax.broadcasted_iota(jnp.int32, (nrow, 128), 1)
    message = (
        jnp.where(lanes == rank_col, land_col, 0)
        + jnp.where(lanes == CAP + rank_col, kind_col, 0)
        + jnp.where(lanes == 2 * CAP + rank_col, live_col, 0)
        + jnp.where(lanes == 3 * CAP + rank_col, src_col, 0)
    )
    for n in range(9):
        idx_send[n] = jnp.sum(jnp.where(code_col == n, message, 0), axis=0, keepdims=True)

    own_copy = pltpu.make_async_copy(idx_send, own_s, own_sem)
    own_copy.start()
    arrived(cell, load_sem.at[3])
    own_copy.wait()
    for n in range(9):
        dst = recv if n == HOME else send
        for r in range(CAP):
            col = own_s[n, 0, 3 * CAP + r]
            dst[n, r : r + 1, :nz] = p[pl.ds(col, 1), :]
            dst[n, CAP + r : CAP + r + 1, :nz] = d[pl.ds(col, 1), :]
            dst[n, r : r + 1, nz:] = s[pl.ds(col, 1), :]
            dst[n, CAP + r : CAP + r + 1, nz:] = s[pl.ds(cells + col, 1), :]

    odd = lax.rem(ix, 2)
    away = 2 * odd - 1

    def ask(dx, dy):
        n = 3 * (dx + 1) + dy + 1
        dev = device(dx, dy)
        remote(idx_send.at[n], idx_s.at[n], is_sem, ir_sem.at[dx + 1], dev).start()
        remote(send.at[n], recv.at[n], fs_sem, fr_sem.at[dx + 1], dev).start()

    @pl.when(first)
    def _():
        pl.semaphore_wait(barrier, 5 + y_odd)
        for dy in (-1, 0, 1):
            ty = wrap(iy + dy)
            t_odd = lax.rem(ty, 2)
            slot = 3 * t_odd + dy + 1
            via = (1, ty + 1 - t_odd)
            remote(idx_send.at[dy + 1], via_i.at[slot], is_sem, vi_sem.at[t_odd], via).start()
            remote(send.at[dy + 1], via_f.at[slot], fs_sem, vf_sem.at[t_odd], via).start()

    @pl.when(~first)
    def _():
        @pl.when(~last)
        def _():
            pl.semaphore_wait(barrier, 8)

        @pl.when(ix == nx - 2)
        def _():
            for dy in (-1, 0, 1):
                signal(here_sem, device(1, dy))

        @pl.when(last)
        def _():
            pl.semaphore_wait(here_sem, 3)

        for dy in (-1, 1, 0):
            ask(away, dy)

    for dy in (-1, 1, 0):
        ask(-away, dy)
    for dy in (-1, 1):
        ask(0, dy)

    for c in loads[6:]:
        c.wait()
    xparts = [(p, 0), (d, 0), (s, 0), (s, cells), (k, 0)]
    yparts = [(p, 0), (d, 0), (s, 0), (s, cx), (k, cx)]

    def xcopy(side, f):
        ref, base = xparts[f]
        at = base + (0 if side == 0 else cells - cy)
        return remote(
            ref.at[pl.ds(at, cy), :], xhalo.at[1 - side, f], xs_sem.at[side], xr_sem.at[1 - side],
            device(-1 if side == 0 else 1, 0),
        )

    for f in range(5):
        ref, base = yparts[f]
        base = base * cy if f >= 3 else base
        for side in range(2):
            off = base + (0 if side == 0 else cy - 1)
            yhalo[2 + side, f] = ref[pl.ds(off, cx, stride=cy), :]

    def ycopy(side):
        return remote(
            yhalo.at[2 + side], yhalo.at[1 - side], ys_sem.at[side], yr_sem.at[1 - side],
            device(0, -1 if side == 0 else 1),
        )

    zmask = lax.broadcasted_iota(jnp.int32, (cy, nz), 1) < nz - 1
    ymask = lax.broadcasted_iota(jnp.int32, (cy, nz), 0) < cy - 1

    def slab(a, carry):
        base = pl.multiple_of(a * cy, cy)
        after = pl.multiple_of(jnp.minimum(a + 1, cx - 1) * cy, cy)

        def at(ref, off):
            return ref[pl.ds(off, cy), :]

        p0, d0 = at(p, base), at(d, base)
        w0, o0 = at(s, base), at(s, cells + base)
        m0 = mobility(w0, o0)
        m1 = mobility(at(s, after), at(s, cells + after))
        tx = jnp.where(a < cx - 1, harmonic(at(k, base), at(k, after)), 0.0)
        fx = flux(p0 - at(p, after), d0 - at(d, after), m0, m1, tx)
        net = [fx[f] - carry[f] for f in range(3)]
        for axis, size, mask, offset in ((0, cy, ymask, cells), (1, nz, zmask, 2 * cells)):
            def up(x):
                return pltpu.roll(x, size - 1, axis)

            kk = at(k, offset + base)
            t = jnp.where(mask, harmonic(kk, up(kk)), 0.0)
            fl = flux(p0 - up(p0), d0 - up(d0), m0, [up(m) for m in m0], t)
            net = [net[f] + (fl[f] - pltpu.roll(fl[f], 1, axis)) for f in range(3)]
        scale = STEP / at(v, base)
        v[pl.ds(base, cy), :] = scale
        now = (w0, o0, 1.0 - w0 - o0)
        for f in range(3):
            out[pl.ds(f * cells + base, cy), :] = now[f] - scale * net[f]
        return tuple(fx)

    zero = jnp.zeros((cy, nz), jnp.float32)
    quarter = cx // 4

    def march(start, stop):
        before = tuple(between[f] for f in range(3)) if start else (zero, zero, zero)
        edge = lax.fori_loop(start, stop, slab, before, unroll=2)
        if stop < cx:
            for f in range(3):
                between[f] = edge[f]

    march(0, quarter)

    def onward(j, dy):
        slot, dev = 3 * j + dy + 1, (nx - 1, wrap(iy - 1 + j))
        return (
            remote(via_i.at[slot], idx_s.at[dy + 1], ws_sem.at[0], ir_sem.at[0], dev),
            remote(via_f.at[slot], recv.at[dy + 1], ws_sem.at[1], fr_sem.at[0], dev),
        )

    @pl.when(relays)
    def _():
        for j in (0, 1):
            pl.semaphore_wait(go_sem.at[j], 1)
            arrived(via_i.at[pl.ds(3 * j, 3)], vi_sem.at[j])
            arrived(via_f.at[pl.ds(3 * j, 3)], vf_sem.at[j])
            for dy in (-1, 0, 1):
                for c in onward(j, dy):
                    c.start()

    march(quarter, 2 * quarter)
    has = ((ix > 0, ix < nx - 1), (iy > 0, iy < ny - 1))
    for side in range(2):
        @pl.when(has[0][side])
        def _():
            for f in range(5):
                xcopy(side, f).start()

        @pl.when(has[1][side])
        def _():
            ycopy(side).start()

    @pl.when(~last)
    def _():
        march(2 * quarter, cx)

    def answer(group, sources):
        first = 3 * group
        for i, ints in enumerate(sources):
            n = first + i
            for r in range(CAP):
                land = ints[n, 0, r]
                kd = ints[n, 0, CAP + r]
                live = ints[n, 0, 2 * CAP + r].astype(jnp.float32)
                loc[n, r : r + 1, :nz] = p[pl.ds(land, 1), :]
                loc[n, CAP + r : CAP + r + 1, :nz] = d[pl.ds(land, 1), :]
                loc[n, r : r + 1, nz:] = s[pl.ds(land, 1), :]
                loc[n, CAP + r : CAP + r + 1, nz:] = s[pl.ds(cells + land, 1), :]
                tloc[n, r : r + 1, :] = table[pl.ds(kd, 1), :] * live

    def flows_of(group):
        rows = pl.ds(3 * group, 3)
        far, here = recv[rows], loc[rows]

        def second(x):
            return pltpu.roll(x, CAP, 1)

        gap = far[:, :, :nz] - here[:, :, :nz]
        fl = flux(
            gap,
            second(gap),
            mobility(far[:, :, nz:], second(far[:, :, nz:])),
            mobility(here[:, :, nz:], second(here[:, :, nz:])),
            tloc[rows],
        )
        for f in range(3):
            back[rows, :, f * nz : (f + 1) * nz] = fl[f][:, :CAP]

    def reply(dx, dy):
        n = 3 * (dx + 1) + dy + 1
        return remote(back.at[n], ret.at[n], bs_sem, br_sem, device(-dx, -dy))

    def serve(dx):
        group = dx + 1
        still = isinstance(dx, int)
        many = 2 if still else 3
        arrived(idx_s.at[pl.ds(3 * group, many)], ir_sem.at[group])
        answer(group, (idx_s, own_s, idx_s) if still else (idx_s,) * 3)
        arrived(recv.at[pl.ds(3 * group, many)], fr_sem.at[group])
        flows_of(group)
        if not still:
            @pl.when(first & (dx == 1))
            def _():
                pl.semaphore_wait(here_sem, 3)

        for dy in (-1, 1) if still else (-1, 1, 0):
            reply(dx, dy).start()

    @pl.when(last)
    def _():
        serve(-away)

    serve(0)
    serve(away)

    @pl.when(~last)
    def _():
        serve(-away)

    @pl.when(last)
    def _():
        march(2 * quarter, cx)

    for side in range(2):
        @pl.when(has[0][side])
        def _():
            arrived(xhalo.at[side], xs_sem.at[side])
            arrived(xhalo.at[side], xr_sem.at[side])
            at = 0 if side == 0 else cells - cy
            mine = [ref[pl.ds(base + at, cy), :] for ref, base in xparts]
            near = [xhalo[side, f] for f in range(5)]
            low, high = (near, mine) if side == 0 else (mine, near)
            fl = edge_flux(low, high)
            scale = v[pl.ds(at, cy), :]
            for f in range(3):
                rows = pl.ds(f * cells + at, cy)
                out[rows, :] = out[rows, :] + (scale * fl[f] if side == 0 else -scale * fl[f])

    for side in range(2):
        @pl.when(has[1][side])
        def _():
            ycopy(side).wait_send()
            ycopy(1 - side).wait_recv()
            at = 0 if side == 0 else cy - 1
            mine = [yhalo[2 + side, f] for f in range(5)]
            near = [yhalo[side, f] for f in range(5)]
            low, high = (near, mine) if side == 0 else (mine, near)
            fl = edge_flux(low, high)
            scale = v[pl.ds(at, cx, stride=cy), :]
            for f in range(3):
                rows = pl.ds(f * cells + at, cx, stride=cy)
                out[rows, :] = out[rows, :] + (scale * fl[f] if side == 0 else -scale * fl[f])

    lane1 = lax.broadcasted_iota(jnp.int32, (1, 128), 1)
    slots = 10 * CAP
    spot = jnp.full((1, 128), -1, jnp.int32)
    for n in range(9):
        for r in range(CAP):
            spot = jnp.where(lane1 == n * CAP + r, (own_s if n == HOME else idx_s)[n, 0, r], spot)
    for r in range(CAP):
        spot = jnp.where(lane1 == 9 * CAP + r, own_s[HOME, 0, 3 * CAP + r], spot)
    spot = jnp.where(lane1 < slots, spot, 0)
    spot = spot + pltpu.roll(spot, slots, 1) + pltpu.roll(spot, 2 * slots, 1)
    flows = jnp.concatenate([-back[n] for n in range(9)] + [back[HOME]], axis=0)
    hi = flows.astype(jnp.bfloat16).astype(jnp.float32)
    rest = flows - hi
    mid = rest.astype(jnp.bfloat16).astype(jnp.float32)
    pad = jnp.zeros((128 - 3 * slots, 3 * nz), jnp.float32)
    parts = jnp.concatenate([hi, mid, rest - mid, pad], axis=0).astype(jnp.bfloat16)
    step = 8 * cy
    for c in range(cells // step):
        ids = lax.broadcasted_iota(jnp.int32, (step, 128), 0) + c * step
        hot = (ids == spot).astype(jnp.float32).astype(jnp.bfloat16)
        add = jnp.dot(hot, parts, preferred_element_type=jnp.float32)
        scale = v[c * step : (c + 1) * step, :]
        for f in range(3):
            at = pl.ds(f * cells + c * step, step)
            out[at, :] = out[at, :] - scale * add[:, f * nz : (f + 1) * nz]

    for n in OTHERS:
        for r in range(CAP):
            scl[n, r : r + 1, :] = v[pl.ds(own_s[n, 0, 3 * CAP + r], 1), :]
    @pl.when(relays)
    def _():
        arrived(via_i, ws_sem.at[0])
        arrived(via_f, ws_sem.at[1])

    arrived(idx_send.at[pl.ds(0, 8)], is_sem)
    arrived(send.at[pl.ds(0, 8)], fs_sem)
    arrived(back.at[pl.ds(0, 8)], bs_sem)
    arrived(ret.at[pl.ds(0, 8)], br_sem)
    for n in OTHERS:
        for f in range(3):
            res[n, :, f * nz : (f + 1) * nz] = ret[n, :, f * nz : (f + 1) * nz] * scl[n]


def finish(cells, nz, part, res_in, own_s, held, res, final, sem):
    for n in OTHERS:
        for r in range(CAP):
            col = own_s[n, 0, 3 * CAP + r]
            for f in range(3):
                row = pl.ds(f * cells + col, 1)
                held[row, :] = held[row, :] - res[n, r : r + 1, f * nz : (f + 1) * nz]
    size = 3 * cells // PIECES
    for i in range(PIECES):
        rows = pl.ds(i * size, size)
        pltpu.make_async_copy(held.at[rows], final.at[rows], sem).start()
    pltpu.make_async_copy(held, final, sem).wait()


def body(pressure, depth, saturation, permeability, pore_volume, pairs, kind, count, table):
    cx, cy, nz = pressure.shape
    nrow = pairs.shape[0]
    kinds = table.shape[0]
    cells = cx * cy
    f32 = jnp.float32
    dma = pltpu.SemaphoreType.DMA
    regular = pltpu.SemaphoreType.REGULAR
    any_spec = pl.BlockSpec(memory_space=pltpu.HBM)
    vmem = pl.BlockSpec(memory_space=pltpu.VMEM)
    smem = pl.BlockSpec(memory_space=pltpu.SMEM)
    part, res, own = pl.pallas_call(
        functools.partial(kernel, cx, cy, nz, nrow),
        out_shape=(
            pltpu.VMEM((3 * cells, nz), f32),
            pltpu.VMEM((9, CAP, 3 * nz), f32),
            pltpu.SMEM((9, 1, 128), jnp.int32),
        ),
        in_specs=[any_spec] * 9,
        out_specs=(vmem, vmem, smem),
        scratch_shapes=[
            pltpu.VMEM((4 * cells, nz), f32),
            pltpu.VMEM((3 * cells, nz), f32),
            pltpu.VMEM((cells, nz), f32),
            pltpu.VMEM((kinds, nz), f32),
            pltpu.VMEM((3, nrow), jnp.int32),
            pltpu.SMEM((1,), jnp.int32),
            pltpu.VMEM((nrow,), jnp.int32),
            pltpu.VMEM((9, 1, 128), jnp.int32),
            pltpu.SMEM((9, 1, 128), jnp.int32),
            pltpu.VMEM((9, ROWS, 2 * nz), f32),
            pltpu.VMEM((9, ROWS, 2 * nz), f32),
            pltpu.VMEM((9, ROWS, 2 * nz), f32),
            pltpu.VMEM((9, ROWS, nz), f32),
            pltpu.VMEM((9, CAP, 3 * nz), f32),
            pltpu.VMEM((9, CAP, 3 * nz), f32),
            pltpu.VMEM((9, CAP, nz), f32),
            pltpu.VMEM((2, 5, cy, nz), f32),
            pltpu.VMEM((4, 5, cx, nz), f32),
            dma((7,)), dma,
            dma, dma((3,)), dma, dma((3,)), dma, dma,
            dma((2,)), dma((2,)), dma((2,)), dma((2,)),
            pltpu.VMEM((3, cy, nz), f32),
            pltpu.VMEM((6, 1, 128), jnp.int32),
            pltpu.VMEM((6, ROWS, 2 * nz), f32),
            dma((2,)), dma((2,)), dma((2,)), regular((2,)), regular,
        ],
        compiler_params=pltpu.CompilerParams(
            collective_id=0, has_side_effects=True, vmem_limit_bytes=60000000
        ),
    )(
        pressure.reshape(cells, nz),
        depth.reshape(cells, nz),
        saturation.reshape(2 * cells, nz),
        permeability.reshape(3 * cells, nz),
        pore_volume.reshape(cells, nz),
        pairs.T,
        kind,
        count,
        table,
    )
    _, _, out = pl.pallas_call(
        functools.partial(finish, cells, nz),
        out_shape=(
            pltpu.VMEM((3 * cells, nz), f32),
            pltpu.VMEM((9, CAP, 3 * nz), f32),
            jax.ShapeDtypeStruct((3 * cells, nz), f32),
        ),
        in_specs=[vmem, vmem, smem],
        out_specs=(vmem, vmem, any_spec),
        scratch_shapes=[dma],
        input_output_aliases={0: 0, 1: 1},
    )(part, res, own)
    return out.reshape(3, cx, cy, nz)


def solution(mesh):
    cell = P("gx", "gy", None)
    cells = P(None, "gx", "gy", None)
    both = ("gx", "gy")
    return jax.shard_map(
        body,
        mesh=mesh,
        in_specs=(cell, cell, cells, cells, cell, P(both, None), P(both), P(both), P()),
        out_specs=cells,
        check_vma=False,
    )
```

```python
import functools

import jax
import jax.numpy as jnp
from jax import lax
from jax.experimental import pallas as pl
from jax.experimental.pallas import tpu as pltpu
from jax.sharding import PartitionSpec as P

CAP = 4
ROWS = 2 * CAP
VISCOSITY = (0.5, 1.0, 0.25)
DENSITY = (1.0, 0.8, 0.25)
STEP = 0.2
MESH = pl.DeviceIdType.MESH
NEAR = [(dx, dy) for dx in (-1, 0, 1) for dy in (-1, 0, 1)]
HOME = 4
OTHERS = [n for n in range(9) if n != HOME]
PIECES = 12


def mobility(w, o):
    g = 1.0 - w - o
    return (w * w * (1.0 / VISCOSITY[0]), o * o, g * g * (1.0 / VISCOSITY[2]))


def harmonic(a, b):
    return 2.0 * a * b / (a + b)


def flux(dp, dd, low, high, trans):
    flows = []
    for f in range(3):
        drive = dp - DENSITY[f] * dd if DENSITY[f] != 1.0 else dp - dd
        flows.append(trans * jnp.where(drive > 0.0, low[f], high[f]) * drive)
    return flows


def edge_flux(low, high):
    return flux(
        low[0] - high[0],
        low[1] - high[1],
        mobility(low[2], low[3]),
        mobility(high[2], high[3]),
        harmonic(low[4], high[4]),
    )


def kernel(
    cx, cy, nz, nrow,
    p_hbm, d_hbm, s_hbm, k_hbm, v_hbm, pairs_hbm, kind_hbm, count_hbm, table_hbm,
    out, res, own_s,
    cell, k, v, table, pairs_v, count_s, kindrow,
    idx_send, idx_s, send, recv, loc, tloc, back, ret, scl,
    xhalo, yhalo,
    ir_sem, fr_sem, br_sem, xr_sem, yr_sem,
    between, via_i, via_f, vi_sem, vf_sem, go_sem, here_sem,
):
    def arrived(ref, sem):
        pltpu.make_async_copy(ref, ref, sem).wait()

    def work(load_sem, own_sem, out_sem, ws_sem, xs_sem, ys_sem):
        nx = lax.axis_size("gx")
        ny = lax.axis_size("gy")
        ix = lax.axis_index("gx")
        iy = lax.axis_index("gy")
        cells = cx * cy
        p, d, s = (cell.at[pl.ds(i * cells, (1, 1, 2)[i] * cells)] for i in range(3))

        def device(dx, dy):
            return (lax.rem(ix + dx + nx, nx), lax.rem(iy + dy + ny, ny))

        def remote(src, dst, ss, rs, dev):
            return pltpu.make_async_remote_copy(
                src_ref=src, dst_ref=dst, send_sem=ss, recv_sem=rs, device_id=dev, device_id_type=MESH
            )

        def signal(sem, dev):
            pl.semaphore_signal(sem, inc=1, device_id=dev, device_id_type=MESH)

        def wrap(y):
            return lax.rem(y + 2 * ny, ny)

        first, last = ix == 0, ix == nx - 1
        y_odd = lax.rem(iy, 2)
        relays = (ix == 1) & (y_odd == 1)
        barrier = pltpu.get_barrier_semaphore()
        for n in OTHERS:
            dx, dy = NEAR[n]
            if dx == 1:
                @pl.when(ix < nx - 2)
                def _():
                    signal(barrier, device(dx, dy))
            elif dx == 0:
                @pl.when(~last)
                def _():
                    signal(barrier, device(dx, dy))
            else:
                signal(barrier, device(dx, dy))

        @pl.when(relays)
        def _():
            signal(barrier, (nx - 1, wrap(iy - 1)))
            signal(barrier, (nx - 1, iy))
            signal(barrier, (0, wrap(iy - 2)))

        loads = [
            pltpu.make_async_copy(src, dst, load_sem.at[i])
            for i, src, dst in (
                (0, pairs_hbm, pairs_v),
                (1, kind_hbm, kindrow),
                (2, count_hbm, count_s),
                (3, p_hbm, p),
                (3, d_hbm, d),
                (3, s_hbm, s),
                (4, k_hbm, k),
                (5, v_hbm, v),
                (6, table_hbm, table),
            )
        ]
        for c in loads:
            c.start()

        @pl.when(last)
        def _():
            pl.semaphore_wait(barrier, 4)
            signal(go_sem.at[y_odd], (1, iy + 1 - y_odd))
            for dy in (-1, 0, 1):
                signal(here_sem, (0, wrap(iy + dy)))

        for c in loads[:3]:
            c.wait()
        lane_of_row = lax.broadcasted_iota(jnp.int32, (nrow, nrow), 1)
        sub_of_row = lax.broadcasted_iota(jnp.int32, (nrow, nrow), 0)
        eye = lane_of_row == sub_of_row
        pv = pairs_v[...]
        tgt_row = pv[1:2, :]

        def to_sublanes(row):
            return jnp.sum(jnp.where(eye, row, 0), axis=1, keepdims=True)

        src_col = to_sublanes(pv[0:1, :])
        tgt_col = to_sublanes(tgt_row)
        land_col = to_sublanes(pv[2:3, :])
        kind_col = to_sublanes(kindrow[...].reshape(1, nrow))
        rank_col = jnp.sum(
            ((tgt_col == tgt_row) & (lane_of_row < sub_of_row)).astype(jnp.int32), axis=1, keepdims=True
        )
        live_col = (lax.broadcasted_iota(jnp.int32, (nrow, 1), 0) < count_s[0]).astype(jnp.int32)
        code_col = jnp.zeros_like(tgt_col)
        for n in range(9):
            hx, hy = device(*NEAR[n])
            code_col = jnp.where(tgt_col == hx * ny + hy, n, code_col)
        lanes = lax.broadcasted_iota(jnp.int32, (nrow, 128), 1)
        message = (
            jnp.where(lanes == rank_col, land_col, 0)
            + jnp.where(lanes == CAP + rank_col, kind_col, 0)
            + jnp.where(lanes == 2 * CAP + rank_col, live_col, 0)
            + jnp.where(lanes == 3 * CAP + rank_col, src_col, 0)
        )
        for n in range(9):
            idx_send[n] = jnp.sum(jnp.where(code_col == n, message, 0), axis=0, keepdims=True)

        own_copy = pltpu.make_async_copy(idx_send, own_s, own_sem)
        own_copy.start()
        arrived(cell, load_sem.at[3])
        own_copy.wait()
        for n in range(9):
            dst = recv if n == HOME else send
            for r in range(CAP):
                col = own_s[n, 0, 3 * CAP + r]
                dst[n, r : r + 1, :nz] = p[pl.ds(col, 1), :]
                dst[n, CAP + r : CAP + r + 1, :nz] = d[pl.ds(col, 1), :]
                dst[n, r : r + 1, nz:] = s[pl.ds(col, 1), :]
                dst[n, CAP + r : CAP + r + 1, nz:] = s[pl.ds(cells + col, 1), :]

        odd = lax.rem(ix, 2)
        away = 2 * odd - 1

        def ask(dx, dy):
            n = 3 * (dx + 1) + dy + 1
            dev = device(dx, dy)
            slot = inbox(dx, dy)
            remote(idx_send.at[n], idx_s.at[n], out_sem, ir_sem.at[slot], dev).start()
            remote(send.at[n], recv.at[n], out_sem, fr_sem.at[slot], dev).start()

        def inbox(dx, dy):
            if isinstance(dx, int):
                return dy + 1 if dx < 0 else 3 + dx
            return jnp.where(dx < 0, dy + 1, 3 + dx)

        def relay_slot(j, off):
            if isinstance(off, int):
                return (0, 1 + j, 3 + j, 5)[off + 2]
            return jnp.where(off == -2, 0, jnp.where(off == -1, 1 + j, jnp.where(off == 0, 3 + j, 5)))

        @pl.when(first)
        def _():
            pl.semaphore_wait(barrier, 5 + y_odd)
            for dy in (-1, 0, 1):
                ty = wrap(iy + dy)
                t_odd = lax.rem(ty, 2)
                off = t_odd - 1 - dy
                slot = relay_slot(t_odd, off)
                via = (1, ty + 1 - t_odd)
                remote(idx_send.at[dy + 1], via_i.at[slot], out_sem, vi_sem.at[off + 2], via).start()
                remote(send.at[dy + 1], via_f.at[slot], out_sem, vf_sem.at[off + 2], via).start()

        @pl.when(~first)
        def _():
            @pl.when(~last)
            def _():
                pl.semaphore_wait(barrier, 8)

            @pl.when(ix == nx - 2)
            def _():
                for dy in (-1, 0, 1):
                    signal(here_sem, device(1, dy))

            @pl.when(last)
            def _():
                pl.semaphore_wait(here_sem, 3)

            for dy in (-1, 1, 0):
                ask(away, dy)

        def near_asks():
            for dy in (-1, 1, 0):
                ask(-away, dy)
            for dy in (-1, 1):
                ask(0, dy)

        @pl.when(~first)
        def _():
            near_asks()

        for c in loads[6:]:
            c.wait()
        xparts = [(p, 0), (d, 0), (s, 0), (s, cells), (k, 0)]
        yparts = [(p, 0), (d, 0), (s, 0), (s, cx), (k, cx)]

        def xcopy(side, f):
            ref, base = xparts[f]
            at = base + (0 if side == 0 else cells - cy)
            return remote(
                ref.at[pl.ds(at, cy), :], xhalo.at[1 - side, f], xs_sem.at[side], xr_sem.at[1 - side],
                device(-1 if side == 0 else 1, 0),
            )

        for f in range(5):
            ref, base = yparts[f]
            base = base * cy if f >= 3 else base
            for side in range(2):
                off = base + (0 if side == 0 else cy - 1)
                yhalo[2 + side, f] = ref[pl.ds(off, cx, stride=cy), :]

        def ycopy(side):
            return remote(
                yhalo.at[2 + side], yhalo.at[1 - side], ys_sem.at[side], yr_sem.at[1 - side],
                device(0, -1 if side == 0 else 1),
            )

        zmask = lax.broadcasted_iota(jnp.int32, (cy, nz), 1) < nz - 1
        ymask = lax.broadcasted_iota(jnp.int32, (cy, nz), 0) < cy - 1

        def slab(a, carry):
            base = pl.multiple_of(a * cy, cy)
            after = pl.multiple_of(jnp.minimum(a + 1, cx - 1) * cy, cy)

            def at(ref, off):
                return ref[pl.ds(off, cy), :]

            p0, d0 = at(p, base), at(d, base)
            w0, o0 = at(s, base), at(s, cells + base)
            m0 = mobility(w0, o0)
            m1 = mobility(at(s, after), at(s, cells + after))
            tx = jnp.where(a < cx - 1, harmonic(at(k, base), at(k, after)), 0.0)
            fx = flux(p0 - at(p, after), d0 - at(d, after), m0, m1, tx)
            net = [fx[f] - carry[f] for f in range(3)]
            for axis, size, mask, offset in ((0, cy, ymask, cells), (1, nz, zmask, 2 * cells)):
                def up(x):
                    return pltpu.roll(x, size - 1, axis)

                kk = at(k, offset + base)
                t = jnp.where(mask, harmonic(kk, up(kk)), 0.0)
                fl = flux(p0 - up(p0), d0 - up(d0), m0, [up(m) for m in m0], t)
                net = [net[f] + (fl[f] - pltpu.roll(fl[f], 1, axis)) for f in range(3)]
            scale = STEP / at(v, base)
            v[pl.ds(base, cy), :] = scale
            now = (w0, o0, 1.0 - w0 - o0)
            for f in range(3):
                out[pl.ds(f * cells + base, cy), :] = now[f] - scale * net[f]
            return tuple(fx)

        zero = jnp.zeros((cy, nz), jnp.float32)
        quarter = cx // 4

        def march(start, stop):
            before = tuple(between[f] for f in range(3)) if start else (zero, zero, zero)
            edge = lax.fori_loop(start, stop, slab, before, unroll=2)
            if stop < cx:
                for f in range(3):
                    between[f] = edge[f]

        march(0, quarter)

        @pl.when(first)
        def _():
            near_asks()

        def take(off):
            start, many = ((0, 1), (1, 2), (3, 2), (5, 1))[off + 2]
            arrived(via_i.at[pl.ds(start, many)], vi_sem.at[off + 2])
            arrived(via_f.at[pl.ds(start, many)], vf_sem.at[off + 2])

        def onward(j, off):
            dy = j - 1 - off
            slot, dev = relay_slot(j, off), (nx - 1, wrap(iy - 1 + j))
            remote(via_i.at[slot], idx_s.at[dy + 1], ws_sem, ir_sem.at[dy + 1], dev).start()
            remote(via_f.at[slot], recv.at[dy + 1], ws_sem, fr_sem.at[dy + 1], dev).start()

        def pass_on(plan):
            for step in plan:
                if step in ("even", "odd"):
                    pl.semaphore_wait(go_sem.at[int(step == "odd")], 1)
                elif isinstance(step, int):
                    take(step)
                else:
                    onward(*step)

        @pl.when(relays & (iy == 1))
        def _():
            pass_on(["even", 0, (0, 0), -1, (0, -1), -2, (0, -2), "odd", (1, -1), (1, 0), 1, (1, 1)])

        @pl.when(relays & (iy != 1))
        def _():
            pass_on(["odd", 1, (1, 1), "even", -2, (0, -2), 0, (0, 0), (1, 0), -1, (0, -1), (1, -1)])

        march(quarter, 2 * quarter)
        has = ((ix > 0, ix < nx - 1), (iy > 0, iy < ny - 1))
        for side in range(2):
            @pl.when(has[0][side])
            def _():
                for f in range(5):
                    xcopy(side, f).start()

            @pl.when(has[1][side])
            def _():
                ycopy(side).start()

        @pl.when(~last)
        def _():
            march(2 * quarter, cx)

        def answer(n, ints):
            for r in range(CAP):
                land = ints[n, 0, r]
                kd = ints[n, 0, CAP + r]
                live = ints[n, 0, 2 * CAP + r].astype(jnp.float32)
                loc[n, r : r + 1, :nz] = p[pl.ds(land, 1), :]
                loc[n, CAP + r : CAP + r + 1, :nz] = d[pl.ds(land, 1), :]
                loc[n, r : r + 1, nz:] = s[pl.ds(land, 1), :]
                loc[n, CAP + r : CAP + r + 1, nz:] = s[pl.ds(cells + land, 1), :]
                tloc[n, r : r + 1, :] = table[pl.ds(kd, 1), :] * live

        def flows_of(start, many):
            rows = pl.ds(start, many)
            far, here = recv[rows], loc[rows]

            def second(x):
                return pltpu.roll(x, CAP, 1)

            gap = far[:, :, :nz] - here[:, :, :nz]
            fl = flux(
                gap,
                second(gap),
                mobility(far[:, :, nz:], second(far[:, :, nz:])),
                mobility(here[:, :, nz:], second(here[:, :, nz:])),
                tloc[rows],
            )
            for f in range(3):
                back[rows, :, f * nz : (f + 1) * nz] = fl[f][:, :CAP]

        def reply(dx, dy):
            n = 3 * (dx + 1) + dy + 1
            return remote(back.at[n], ret.at[n], out_sem, br_sem, device(-dx, -dy))

        def landed(buf, sem, dx):
            start = 3 * (dx + 1)
            if dx < 0:
                for i in range(3):
                    arrived(buf.at[i], sem.at[i])
            else:
                arrived(buf.at[pl.ds(start, 2 + dx)], sem.at[3 + dx])

        def serve(dx):
            start = 3 * (dx + 1)
            landed(idx_s, ir_sem, dx)
            for i in range(3):
                answer(start + i, own_s if start + i == HOME else idx_s)
            landed(recv, fr_sem, dx)
            flows_of(start, 3)
            if dx == 1:
                @pl.when(first)
                def _():
                    pl.semaphore_wait(here_sem, 3)

            for dy in (-1, 1, 0):
                if dx or dy:
                    reply(dx, dy).start()

        @pl.when(last)
        def _():
            side = jnp.where((iy == 0) | (iy == ny - 1), -1, 1)
            for dy in (side, 0, -side):
                n = dy + 1
                arrived(idx_s.at[n], ir_sem.at[n])
                answer(n, idx_s)
                arrived(recv.at[n], fr_sem.at[n])
                flows_of(n, 1)
                reply(-1, dy).start()

        serve(0)

        @pl.when(odd == 1)
        def _():
            serve(1)

        @pl.when(~last)
        def _():
            serve(-1)

        @pl.when(odd == 0)
        def _():
            serve(1)

        @pl.when(last)
        def _():
            march(2 * quarter, cx)

        for side in range(2):
            @pl.when(has[0][side])
            def _():
                arrived(xhalo.at[side], xs_sem.at[side])
                arrived(xhalo.at[side], xr_sem.at[side])
                at = 0 if side == 0 else cells - cy
                mine = [ref[pl.ds(base + at, cy), :] for ref, base in xparts]
                near = [xhalo[side, f] for f in range(5)]
                low, high = (near, mine) if side == 0 else (mine, near)
                fl = edge_flux(low, high)
                scale = v[pl.ds(at, cy), :]
                for f in range(3):
                    rows = pl.ds(f * cells + at, cy)
                    out[rows, :] = out[rows, :] + (scale * fl[f] if side == 0 else -scale * fl[f])

        for side in range(2):
            @pl.when(has[1][side])
            def _():
                ycopy(side).wait_send()
                ycopy(1 - side).wait_recv()
                at = 0 if side == 0 else cy - 1
                mine = [yhalo[2 + side, f] for f in range(5)]
                near = [yhalo[side, f] for f in range(5)]
                low, high = (near, mine) if side == 0 else (mine, near)
                fl = edge_flux(low, high)
                scale = v[pl.ds(at, cx, stride=cy), :]
                for f in range(3):
                    rows = pl.ds(f * cells + at, cx, stride=cy)
                    out[rows, :] = out[rows, :] + (scale * fl[f] if side == 0 else -scale * fl[f])

        lane1 = lax.broadcasted_iota(jnp.int32, (1, 128), 1)
        slots = 10 * CAP
        spot = jnp.full((1, 128), -1, jnp.int32)
        for n in range(9):
            for r in range(CAP):
                spot = jnp.where(lane1 == n * CAP + r, (own_s if n == HOME else idx_s)[n, 0, r], spot)
        for r in range(CAP):
            spot = jnp.where(lane1 == 9 * CAP + r, own_s[HOME, 0, 3 * CAP + r], spot)
        spot = jnp.where(lane1 < slots, spot, 0)
        spot = spot + pltpu.roll(spot, slots, 1) + pltpu.roll(spot, 2 * slots, 1)
        flows = jnp.concatenate([-back[n] for n in range(9)] + [back[HOME]], axis=0)
        hi = flows.astype(jnp.bfloat16).astype(jnp.float32)
        rest = flows - hi
        mid = rest.astype(jnp.bfloat16).astype(jnp.float32)
        pad = jnp.zeros((128 - 3 * slots, 3 * nz), jnp.float32)
        parts = jnp.concatenate([hi, mid, rest - mid, pad], axis=0).astype(jnp.bfloat16)
        step = 8 * cy
        for c in range(cells // step):
            ids = lax.broadcasted_iota(jnp.int32, (step, 128), 0) + c * step
            hot = (ids == spot).astype(jnp.float32).astype(jnp.bfloat16)
            add = jnp.dot(hot, parts, preferred_element_type=jnp.float32)
            scale = v[c * step : (c + 1) * step, :]
            for f in range(3):
                at = pl.ds(f * cells + c * step, step)
                out[at, :] = out[at, :] - scale * add[:, f * nz : (f + 1) * nz]

        for n in OTHERS:
            for r in range(CAP):
                scl[n, r : r + 1, :] = v[pl.ds(own_s[n, 0, 3 * CAP + r], 1), :]
        @pl.when(relays)
        def _():
            arrived(cell.at[pl.ds(0, 6 * (1 + 2 * ROWS))], ws_sem)

        arrived(cell.at[pl.ds(0, 8 * (1 + 2 * ROWS + 3 * CAP))], out_sem)
    dma = pltpu.SemaphoreType.DMA
    pl.run_scoped(work, dma((7,)), dma, dma, dma, dma((2,)), dma((2,)))
    arrived(ret.at[pl.ds(0, 8)], br_sem)
    for n in OTHERS:
        for f in range(3):
            res[n, :, f * nz : (f + 1) * nz] = ret[n, :, f * nz : (f + 1) * nz] * scl[n]


def finish(cells, nz, part, res_in, own_s, held, res, final, sem):
    for n in OTHERS:
        for r in range(CAP):
            col = own_s[n, 0, 3 * CAP + r]
            for f in range(3):
                row = pl.ds(f * cells + col, 1)
                held[row, :] = held[row, :] - res[n, r : r + 1, f * nz : (f + 1) * nz]
    size = 3 * cells // PIECES
    for i in range(PIECES):
        rows = pl.ds(i * size, size)
        pltpu.make_async_copy(held.at[rows], final.at[rows], sem).start()
    pltpu.make_async_copy(held, final, sem).wait()


def body(pressure, depth, saturation, permeability, pore_volume, pairs, kind, count, table):
    cx, cy, nz = pressure.shape
    nrow = pairs.shape[0]
    kinds = table.shape[0]
    cells = cx * cy
    f32 = jnp.float32
    dma = pltpu.SemaphoreType.DMA
    regular = pltpu.SemaphoreType.REGULAR
    any_spec = pl.BlockSpec(memory_space=pltpu.HBM)
    vmem = pl.BlockSpec(memory_space=pltpu.VMEM)
    smem = pl.BlockSpec(memory_space=pltpu.SMEM)
    part, res, own = pl.pallas_call(
        functools.partial(kernel, cx, cy, nz, nrow),
        out_shape=(
            pltpu.VMEM((3 * cells, nz), f32),
            pltpu.VMEM((9, CAP, 3 * nz), f32),
            pltpu.SMEM((9, 1, 128), jnp.int32),
        ),
        in_specs=[any_spec] * 9,
        out_specs=(vmem, vmem, smem),
        scratch_shapes=[
            pltpu.VMEM((4 * cells, nz), f32),
            pltpu.VMEM((3 * cells, nz), f32),
            pltpu.VMEM((cells, nz), f32),
            pltpu.VMEM((kinds, nz), f32),
            pltpu.VMEM((3, nrow), jnp.int32),
            pltpu.SMEM((1,), jnp.int32),
            pltpu.VMEM((nrow,), jnp.int32),
            pltpu.VMEM((9, 1, 128), jnp.int32),
            pltpu.SMEM((9, 1, 128), jnp.int32),
            pltpu.VMEM((9, ROWS, 2 * nz), f32),
            pltpu.VMEM((9, ROWS, 2 * nz), f32),
            pltpu.VMEM((9, ROWS, 2 * nz), f32),
            pltpu.VMEM((9, ROWS, nz), f32),
            pltpu.VMEM((9, CAP, 3 * nz), f32),
            pltpu.VMEM((9, CAP, 3 * nz), f32),
            pltpu.VMEM((9, CAP, nz), f32),
            pltpu.VMEM((2, 5, cy, nz), f32),
            pltpu.VMEM((4, 5, cx, nz), f32),
            dma((5,)), dma((5,)), dma, dma((2,)), dma((2,)),
            pltpu.VMEM((3, cy, nz), f32),
            pltpu.VMEM((6, 1, 128), jnp.int32),
            pltpu.VMEM((6, ROWS, 2 * nz), f32),
            dma((4,)), dma((4,)), regular((2,)), regular,
        ],
        compiler_params=pltpu.CompilerParams(
            collective_id=0, has_side_effects=True, vmem_limit_bytes=60000000
        ),
    )(
        pressure.reshape(cells, nz),
        depth.reshape(cells, nz),
        saturation.reshape(2 * cells, nz),
        permeability.reshape(3 * cells, nz),
        pore_volume.reshape(cells, nz),
        pairs.T,
        kind,
        count,
        table,
    )
    _, _, out = pl.pallas_call(
        functools.partial(finish, cells, nz),
        out_shape=(
            pltpu.VMEM((3 * cells, nz), f32),
            pltpu.VMEM((9, CAP, 3 * nz), f32),
            jax.ShapeDtypeStruct((3 * cells, nz), f32),
        ),
        in_specs=[vmem, vmem, smem],
        out_specs=(vmem, vmem, any_spec),
        scratch_shapes=[dma],
        input_output_aliases={0: 0, 1: 1},
    )(part, res, own)
    return out.reshape(3, cx, cy, nz)


def solution(mesh):
    cell = P("gx", "gy", None)
    cells = P(None, "gx", "gy", None)
    both = ("gx", "gy")
    return jax.shard_map(
        body,
        mesh=mesh,
        in_specs=(cell, cell, cells, cells, cell, P(both, None), P(both), P(both), P()),
        out_specs=cells,
        check_vma=False,
    )
```

```python
import functools

import jax
import jax.numpy as jnp
from jax import lax
from jax.experimental import pallas as pl
from jax.experimental.pallas import tpu as pltpu
from jax.sharding import PartitionSpec as P

CAP = 4
ROWS = 2 * CAP
VISCOSITY = (0.5, 1.0, 0.25)
DENSITY = (1.0, 0.8, 0.25)
STEP = 0.2
MESH = pl.DeviceIdType.MESH
NEAR = [(dx, dy) for dx in (-1, 0, 1) for dy in ((-1, 1, 0) if dx == 0 else (-1, 0, 1))]
HOME = 5
OTHERS = [n for n in range(9) if n != HOME]
PIECES = 12


def mobility(w, o):
    g = 1.0 - w - o
    return (w * w * (1.0 / VISCOSITY[0]), o * o, g * g * (1.0 / VISCOSITY[2]))


def harmonic(a, b):
    return 2.0 * a * b / (a + b)


def flux(dp, dd, low, high, trans):
    flows = []
    for f in range(3):
        drive = dp - DENSITY[f] * dd if DENSITY[f] != 1.0 else dp - dd
        flows.append(trans * jnp.where(drive > 0.0, low[f], high[f]) * drive)
    return flows


def edge_flux(low, high):
    return flux(
        low[0] - high[0],
        low[1] - high[1],
        mobility(low[2], low[3]),
        mobility(high[2], high[3]),
        harmonic(low[4], high[4]),
    )


def kernel(
    cx, cy, nz, nrow,
    p_hbm, d_hbm, s_hbm, k_hbm, v_hbm, pairs_hbm, kind_hbm, count_hbm, table_hbm,
    out, res, own_s,
    cell, k, v, table, pairs_v, count_s, kindrow,
    idx_send, idx_s, send, recv, loc, tloc, back, ret, scl,
    xhalo, yhalo,
    ir_sem, fr_sem, br_sem, xr_sem, yr_sem,
    between, via_i, via_f, vi_sem, vf_sem, go_sem, here_sem, near_sem,
):
    def arrived(ref, sem):
        pltpu.make_async_copy(ref, ref, sem).wait()

    def seat(n):
        return n - 1 if isinstance(n, int) and n > HOME else n

    def work(load_sem, own_sem, out_sem, ws_sem, xs_sem, ys_sem):
        nx = lax.axis_size("gx")
        ny = lax.axis_size("gy")
        ix = lax.axis_index("gx")
        iy = lax.axis_index("gy")
        cells = cx * cy
        p, d, s = (cell.at[pl.ds(i * cells, (1, 1, 2)[i] * cells)] for i in range(3))

        def device(dx, dy):
            return (lax.rem(ix + dx + nx, nx), lax.rem(iy + dy + ny, ny))

        def remote(src, dst, ss, rs, dev):
            return pltpu.make_async_remote_copy(
                src_ref=src, dst_ref=dst, send_sem=ss, recv_sem=rs, device_id=dev, device_id_type=MESH
            )

        def signal(sem, dev):
            pl.semaphore_signal(sem, inc=1, device_id=dev, device_id_type=MESH)

        def wrap(y):
            return lax.rem(y + 2 * ny, ny)

        first, last = ix == 0, ix == nx - 1
        y_odd = lax.rem(iy, 2)
        relays = (ix == 1) & (y_odd == 1)
        barrier = pltpu.get_barrier_semaphore()
        for n in OTHERS:
            dx, dy = NEAR[n]
            if dx == 1:
                @pl.when(ix < nx - 2)
                def _():
                    signal(barrier, device(dx, dy))
            elif dx == 0:
                @pl.when(~first & ~last)
                def _():
                    signal(barrier, device(dx, dy))
            else:
                @pl.when((ix > 1) | relays)
                def _():
                    signal(barrier, device(dx, dy))

        @pl.when(first & (y_odd == 1))
        def _():
            signal(barrier, (1, wrap(iy + 2)))

        @pl.when(relays)
        def _():
            signal(barrier, (nx - 1, wrap(iy - 1)))
            signal(barrier, (nx - 1, iy))
            signal(barrier, (0, wrap(iy - 2)))

        @pl.when(last)
        def _():
            pl.semaphore_wait(barrier, 1)
            signal(go_sem.at[y_odd], (1, iy + 1 - y_odd))

        loads = [
            pltpu.make_async_copy(src, dst, load_sem.at[i])
            for i, src, dst in (
                (0, pairs_hbm, pairs_v),
                (1, kind_hbm, kindrow),
                (2, count_hbm, count_s),
                (3, p_hbm, p),
                (3, d_hbm, d),
                (3, s_hbm, s),
                (4, k_hbm, k),
                (5, v_hbm, v),
                (6, table_hbm, table),
            )
        ]
        for c in loads:
            c.start()

        for c in loads[:3]:
            c.wait()
        lane_of_row = lax.broadcasted_iota(jnp.int32, (nrow, nrow), 1)
        sub_of_row = lax.broadcasted_iota(jnp.int32, (nrow, nrow), 0)
        eye = lane_of_row == sub_of_row
        pv = pairs_v[...]
        tgt_row = pv[1:2, :]

        def to_sublanes(row):
            return jnp.sum(jnp.where(eye, row, 0), axis=1, keepdims=True)

        src_col = to_sublanes(pv[0:1, :])
        tgt_col = to_sublanes(tgt_row)
        land_col = to_sublanes(pv[2:3, :])
        kind_col = to_sublanes(kindrow[...].reshape(1, nrow))
        rank_col = jnp.sum(
            ((tgt_col == tgt_row) & (lane_of_row < sub_of_row)).astype(jnp.int32), axis=1, keepdims=True
        )
        live_col = (lax.broadcasted_iota(jnp.int32, (nrow, 1), 0) < count_s[0]).astype(jnp.int32)
        code_col = jnp.zeros_like(tgt_col)
        for n in range(9):
            hx, hy = device(*NEAR[n])
            code_col = jnp.where(tgt_col == hx * ny + hy, n, code_col)
        lanes = lax.broadcasted_iota(jnp.int32, (nrow, 128), 1)
        message = (
            jnp.where(lanes == rank_col, land_col, 0)
            + jnp.where(lanes == CAP + rank_col, kind_col, 0)
            + jnp.where(lanes == 2 * CAP + rank_col, live_col, 0)
            + jnp.where(lanes == 3 * CAP + rank_col, src_col, 0)
        )
        for n in range(9):
            idx_send[n] = jnp.sum(jnp.where(code_col == n, message, 0), axis=0, keepdims=True)

        own_copy = pltpu.make_async_copy(idx_send, own_s, own_sem)
        own_copy.start()
        arrived(cell, load_sem.at[3])
        own_copy.wait()
        for n in range(9):
            dst = recv if n == HOME else send
            for r in range(CAP):
                col = own_s[n, 0, 3 * CAP + r]
                dst[n, r : r + 1, :nz] = p[pl.ds(col, 1), :]
                dst[n, CAP + r : CAP + r + 1, :nz] = d[pl.ds(col, 1), :]
                dst[n, r : r + 1, nz:] = s[pl.ds(col, 1), :]
                dst[n, CAP + r : CAP + r + 1, nz:] = s[pl.ds(cells + col, 1), :]

        odd = lax.rem(ix, 2)
        away = 2 * odd - 1

        def place(dx, dy):
            if isinstance(dx, int) and dx == 0:
                return NEAR.index((0, dy))
            return 3 * (dx + 1) + dy + 1

        def ask(dx, dy):
            n = place(dx, dy)
            dev = device(dx, dy)
            slot = inbox(dx, dy)
            remote(idx_send.at[n], idx_s.at[n], out_sem, ir_sem.at[slot], dev).start()
            remote(send.at[n], recv.at[n], out_sem, fr_sem.at[slot], dev).start()

        def inbox(dx, dy):
            if isinstance(dx, int):
                return dy + 1 if dx < 0 else 3 + dx
            return jnp.where(dx < 0, dy + 1, 3 + dx)

        def relay_slot(j, off):
            if isinstance(off, int):
                return (0, 1 + j, 3 + j, 5)[off + 2]
            return jnp.where(off == -2, 0, jnp.where(off == -1, 1 + j, jnp.where(off == 0, 3 + j, 5)))

        def far_asks():
            for dy in (-1, 1, 0):
                ask(away, dy)

        def near_asks():
            for dy in (-1, 1, 0):
                ask(-away, dy)
            for dy in (-1, 1):
                ask(0, dy)

        @pl.when(first)
        def _():
            pl.semaphore_wait(barrier, 2)
            for dy in (-1, 0, 1):
                ty = wrap(iy + dy)
                t_odd = lax.rem(ty, 2)
                off = t_odd - 1 - dy
                slot = relay_slot(t_odd, off)
                via = (1, ty + 1 - t_odd)
                remote(idx_send.at[dy + 1], via_i.at[slot], out_sem, vi_sem.at[off + 2], via).start()
                remote(send.at[dy + 1], via_f.at[slot], out_sem, vf_sem.at[off + 2], via).start()

        @pl.when(~first)
        def _():
            @pl.when(~last)
            def _():
                pl.semaphore_wait(barrier, 8 + relays.astype(jnp.int32))

            @pl.when(relays)
            def _():
                signal(barrier, (nx - 1, wrap(iy - 1)))
                signal(barrier, (nx - 1, iy))
                for off in (-2, -1, 0, 1):
                    signal(near_sem, (0, wrap(iy + off)))

            @pl.when(ix == nx - 2)
            def _():
                for dy in (-1, 0, 1):
                    signal(here_sem, device(1, dy))

            @pl.when(last)
            def _():
                pl.semaphore_wait(barrier, 1)
                for dy in (-1, 0, 1):
                    signal(here_sem, device(1, dy))
                pl.semaphore_wait(here_sem, 3)

            @pl.when(ix != 2)
            def _():
                far_asks()

        @pl.when(~first & (ix != 2))
        def _():
            near_asks()

        for c in loads[6:]:
            c.wait()
        xparts = [(p, 0), (d, 0), (s, 0), (s, cells), (k, 0)]
        yparts = [(p, 0), (d, 0), (s, 0), (s, cx), (k, cx)]

        def xcopy(side, f):
            ref, base = xparts[f]
            at = base + (0 if side == 0 else cells - cy)
            return remote(
                ref.at[pl.ds(at, cy), :], xhalo.at[1 - side, f], xs_sem.at[side], xr_sem.at[1 - side],
                device(-1 if side == 0 else 1, 0),
            )

        for f in range(5):
            ref, base = yparts[f]
            base = base * cy if f >= 3 else base
            for side in range(2):
                off = base + (0 if side == 0 else cy - 1)
                yhalo[2 + side, f] = ref[pl.ds(off, cx, stride=cy), :]

        def ycopy(side):
            return remote(
                yhalo.at[2 + side], yhalo.at[1 - side], ys_sem.at[side], yr_sem.at[1 - side],
                device(0, -1 if side == 0 else 1),
            )

        zmask = lax.broadcasted_iota(jnp.int32, (cy, nz), 1) < nz - 1
        ymask = lax.broadcasted_iota(jnp.int32, (cy, nz), 0) < cy - 1

        def slab(a, carry):
            base = pl.multiple_of(a * cy, cy)
            after = pl.multiple_of(jnp.minimum(a + 1, cx - 1) * cy, cy)

            def at(ref, off):
                return ref[pl.ds(off, cy), :]

            p0, d0 = at(p, base), at(d, base)
            w0, o0 = at(s, base), at(s, cells + base)
            m0 = mobility(w0, o0)
            m1 = mobility(at(s, after), at(s, cells + after))
            tx = jnp.where(a < cx - 1, harmonic(at(k, base), at(k, after)), 0.0)
            fx = flux(p0 - at(p, after), d0 - at(d, after), m0, m1, tx)
            net = [fx[f] - carry[f] for f in range(3)]
            for axis, size, mask, offset in ((0, cy, ymask, cells), (1, nz, zmask, 2 * cells)):
                def up(x):
                    return pltpu.roll(x, size - 1, axis)

                kk = at(k, offset + base)
                t = jnp.where(mask, harmonic(kk, up(kk)), 0.0)
                fl = flux(p0 - up(p0), d0 - up(d0), m0, [up(m) for m in m0], t)
                net = [net[f] + (fl[f] - pltpu.roll(fl[f], 1, axis)) for f in range(3)]
            scale = STEP / at(v, base)
            v[pl.ds(base, cy), :] = scale
            now = (w0, o0, 1.0 - w0 - o0)
            for f in range(3):
                out[pl.ds(f * cells + base, cy), :] = now[f] - scale * net[f]
            return tuple(fx)

        zero = jnp.zeros((cy, nz), jnp.float32)
        quarter = cx // 4

        def march(start, stop):
            before = tuple(between[f] for f in range(3)) if start else (zero, zero, zero)
            edge = lax.fori_loop(start, stop, slab, before, unroll=2)
            if stop < cx:
                for f in range(3):
                    between[f] = edge[f]

        march(0, quarter)

        @pl.when(ix == 2)
        def _():
            far_asks()

        @pl.when(first)
        def _():
            pl.semaphore_wait(near_sem, 2)

        @pl.when(first | (ix == 2))
        def _():
            near_asks()

        def take(off):
            start, many = ((0, 1), (1, 2), (3, 2), (5, 1))[off + 2]
            arrived(via_i.at[pl.ds(start, many)], vi_sem.at[off + 2])
            arrived(via_f.at[pl.ds(start, many)], vf_sem.at[off + 2])

        def onward(j, off):
            dy = j - 1 - off
            slot, dev = relay_slot(j, off), (nx - 1, wrap(iy - 1 + j))
            remote(via_i.at[slot], idx_s.at[dy + 1], ws_sem, ir_sem.at[dy + 1], dev).start()
            remote(via_f.at[slot], recv.at[dy + 1], ws_sem, fr_sem.at[dy + 1], dev).start()

        def pass_on(plan):
            for step in plan:
                if step in ("even", "odd"):
                    pl.semaphore_wait(go_sem.at[int(step == "odd")], 1)
                elif isinstance(step, int):
                    take(step)
                else:
                    onward(*step)

        @pl.when(relays & (iy == 1))
        def _():
            pass_on(["odd", "even", 0, (0, 0), (1, 0), -1, (0, -1), (1, -1), -2, (0, -2), 1, (1, 1)])

        @pl.when(relays & (iy != 1))
        def _():
            pass_on(["even", -2, (0, -2), "odd", 1, (1, 1), 0, (0, 0), (1, 0), -1, (0, -1), (1, -1)])

        march(quarter, 2 * quarter)
        has = ((ix > 0, ix < nx - 1), (iy > 0, iy < ny - 1))
        for side in range(2):
            @pl.when(has[0][side])
            def _():
                for f in range(5):
                    xcopy(side, f).start()

            @pl.when(has[1][side])
            def _():
                ycopy(side).start()

        @pl.when(~last)
        def _():
            march(2 * quarter, cx)

        def answer(n, ints):
            for r in range(CAP):
                land = ints[n, 0, r]
                kd = ints[n, 0, CAP + r]
                live = ints[n, 0, 2 * CAP + r].astype(jnp.float32)
                loc[n, r : r + 1, :nz] = p[pl.ds(land, 1), :]
                loc[n, CAP + r : CAP + r + 1, :nz] = d[pl.ds(land, 1), :]
                loc[n, r : r + 1, nz:] = s[pl.ds(land, 1), :]
                loc[n, CAP + r : CAP + r + 1, nz:] = s[pl.ds(cells + land, 1), :]
                tloc[n, r : r + 1, :] = table[pl.ds(kd, 1), :] * live

        def flows_of(start, many):
            rows = pl.ds(start, many)
            far, here = recv[rows], loc[rows]

            def second(x):
                return pltpu.roll(x, CAP, 1)

            gap = far[:, :, :nz] - here[:, :, :nz]
            fl = flux(
                gap,
                second(gap),
                mobility(far[:, :, nz:], second(far[:, :, nz:])),
                mobility(here[:, :, nz:], second(here[:, :, nz:])),
                tloc[rows],
            )
            for f in range(3):
                back[rows, :, f * nz : (f + 1) * nz] = fl[f][:, :CAP]

        def reply(dx, dy):
            n = place(dx, dy)
            return remote(back.at[n], ret.at[seat(n)], out_sem, br_sem, device(-dx, -dy))

        def landed(buf, sem, dx):
            start = 3 * (dx + 1)
            if dx < 0:
                for i in range(3):
                    arrived(buf.at[i], sem.at[i])
            else:
                arrived(buf.at[pl.ds(start, 2 + dx)], sem.at[3 + dx])

        def serve(dx):
            start = 3 * (dx + 1)
            landed(idx_s, ir_sem, dx)
            for i in range(3):
                answer(start + i, own_s if start + i == HOME else idx_s)
            landed(recv, fr_sem, dx)
            flows_of(start, 3)
            if dx == 1:
                @pl.when(first)
                def _():
                    pl.semaphore_wait(here_sem, 3)

            for dy in (-1, 1, 0):
                if dx or dy:
                    reply(dx, dy).start()

        @pl.when(last)
        def _():
            side = jnp.where((iy == 0) | (iy == ny - 1), -1, 1)
            for dy in (side, 0, -side):
                n = dy + 1
                arrived(idx_s.at[n], ir_sem.at[n])
                answer(n, idx_s)
                arrived(recv.at[n], fr_sem.at[n])
                flows_of(n, 1)
                reply(-1, dy).start()

        serve(0)

        @pl.when(odd == 1)
        def _():
            serve(1)

        @pl.when(~last)
        def _():
            serve(-1)

        @pl.when(odd == 0)
        def _():
            serve(1)

        @pl.when(last)
        def _():
            march(2 * quarter, cx)

        for side in range(2):
            @pl.when(has[0][side])
            def _():
                arrived(xhalo.at[side], xs_sem.at[side])
                arrived(xhalo.at[side], xr_sem.at[side])
                at = 0 if side == 0 else cells - cy
                mine = [ref[pl.ds(base + at, cy), :] for ref, base in xparts]
                near = [xhalo[side, f] for f in range(5)]
                low, high = (near, mine) if side == 0 else (mine, near)
                fl = edge_flux(low, high)
                scale = v[pl.ds(at, cy), :]
                for f in range(3):
                    rows = pl.ds(f * cells + at, cy)
                    out[rows, :] = out[rows, :] + (scale * fl[f] if side == 0 else -scale * fl[f])

        for side in range(2):
            @pl.when(has[1][side])
            def _():
                ycopy(side).wait_send()
                ycopy(1 - side).wait_recv()
                at = 0 if side == 0 else cy - 1
                mine = [yhalo[2 + side, f] for f in range(5)]
                near = [yhalo[side, f] for f in range(5)]
                low, high = (near, mine) if side == 0 else (mine, near)
                fl = edge_flux(low, high)
                scale = v[pl.ds(at, cx, stride=cy), :]
                for f in range(3):
                    rows = pl.ds(f * cells + at, cx, stride=cy)
                    out[rows, :] = out[rows, :] + (scale * fl[f] if side == 0 else -scale * fl[f])

        lane1 = lax.broadcasted_iota(jnp.int32, (1, 128), 1)
        slots = 10 * CAP
        spot = jnp.full((1, 128), -1, jnp.int32)
        for n in range(9):
            for r in range(CAP):
                spot = jnp.where(lane1 == n * CAP + r, (own_s if n == HOME else idx_s)[n, 0, r], spot)
        for r in range(CAP):
            spot = jnp.where(lane1 == 9 * CAP + r, own_s[HOME, 0, 3 * CAP + r], spot)
        spot = jnp.where(lane1 < slots, spot, 0)
        spot = spot + pltpu.roll(spot, slots, 1) + pltpu.roll(spot, 2 * slots, 1)
        flows = jnp.concatenate([-back[n] for n in range(9)] + [back[HOME]], axis=0)
        hi = flows.astype(jnp.bfloat16).astype(jnp.float32)
        rest = flows - hi
        mid = rest.astype(jnp.bfloat16).astype(jnp.float32)
        pad = jnp.zeros((128 - 3 * slots, 3 * nz), jnp.float32)
        parts = jnp.concatenate([hi, mid, rest - mid, pad], axis=0).astype(jnp.bfloat16)
        step = 8 * cy
        for c in range(cells // step):
            ids = lax.broadcasted_iota(jnp.int32, (step, 128), 0) + c * step
            hot = (ids == spot).astype(jnp.float32).astype(jnp.bfloat16)
            add = jnp.dot(hot, parts, preferred_element_type=jnp.float32)
            scale = v[c * step : (c + 1) * step, :]
            for f in range(3):
                at = pl.ds(f * cells + c * step, step)
                out[at, :] = out[at, :] - scale * add[:, f * nz : (f + 1) * nz]

        for n in OTHERS:
            for r in range(CAP):
                scl[n, r : r + 1, :] = v[pl.ds(own_s[n, 0, 3 * CAP + r], 1), :]
        @pl.when(relays)
        def _():
            arrived(cell.at[pl.ds(0, 6 * (1 + 2 * ROWS))], ws_sem)

        arrived(cell.at[pl.ds(0, 8 * (1 + 2 * ROWS + 3 * CAP))], out_sem)
    dma = pltpu.SemaphoreType.DMA
    pl.run_scoped(work, dma((7,)), dma, dma, dma, dma((2,)), dma((2,)))
    arrived(ret, br_sem)
    for n in OTHERS:
        for f in range(3):
            res[n, :, f * nz : (f + 1) * nz] = ret[seat(n), :, f * nz : (f + 1) * nz] * scl[n]


def finish(cells, nz, part, res_in, own_s, held, res, final, sem):
    for n in OTHERS:
        for r in range(CAP):
            col = own_s[n, 0, 3 * CAP + r]
            for f in range(3):
                row = pl.ds(f * cells + col, 1)
                held[row, :] = held[row, :] - res[n, r : r + 1, f * nz : (f + 1) * nz]
    size = 3 * cells // PIECES
    for i in range(PIECES):
        rows = pl.ds(i * size, size)
        pltpu.make_async_copy(held.at[rows], final.at[rows], sem).start()
    pltpu.make_async_copy(held, final, sem).wait()


def body(pressure, depth, saturation, permeability, pore_volume, pairs, kind, count, table):
    cx, cy, nz = pressure.shape
    nrow = pairs.shape[0]
    kinds = table.shape[0]
    cells = cx * cy
    f32 = jnp.float32
    dma = pltpu.SemaphoreType.DMA
    regular = pltpu.SemaphoreType.REGULAR
    any_spec = pl.BlockSpec(memory_space=pltpu.HBM)
    vmem = pl.BlockSpec(memory_space=pltpu.VMEM)
    smem = pl.BlockSpec(memory_space=pltpu.SMEM)
    part, res, own = pl.pallas_call(
        functools.partial(kernel, cx, cy, nz, nrow),
        out_shape=(
            pltpu.VMEM((3 * cells, nz), f32),
            pltpu.VMEM((9, CAP, 3 * nz), f32),
            pltpu.SMEM((9, 1, 128), jnp.int32),
        ),
        in_specs=[any_spec] * 9,
        out_specs=(vmem, vmem, smem),
        scratch_shapes=[
            pltpu.VMEM((4 * cells, nz), f32),
            pltpu.VMEM((3 * cells, nz), f32),
            pltpu.VMEM((cells, nz), f32),
            pltpu.VMEM((kinds, nz), f32),
            pltpu.VMEM((3, nrow), jnp.int32),
            pltpu.SMEM((1,), jnp.int32),
            pltpu.VMEM((nrow,), jnp.int32),
            pltpu.VMEM((9, 1, 128), jnp.int32),
            pltpu.SMEM((9, 1, 128), jnp.int32),
            pltpu.VMEM((9, ROWS, 2 * nz), f32),
            pltpu.VMEM((9, ROWS, 2 * nz), f32),
            pltpu.VMEM((9, ROWS, 2 * nz), f32),
            pltpu.VMEM((9, ROWS, nz), f32),
            pltpu.VMEM((9, CAP, 3 * nz), f32),
            pltpu.VMEM((8, CAP, 3 * nz), f32),
            pltpu.VMEM((9, CAP, nz), f32),
            pltpu.VMEM((2, 5, cy, nz), f32),
            pltpu.VMEM((4, 5, cx, nz), f32),
            dma((5,)), dma((5,)), dma, dma((2,)), dma((2,)),
            pltpu.VMEM((3, cy, nz), f32),
            pltpu.VMEM((6, 1, 128), jnp.int32),
            pltpu.VMEM((6, ROWS, 2 * nz), f32),
            dma((4,)), dma((4,)), regular((2,)), regular, regular,
        ],
        compiler_params=pltpu.CompilerParams(
            collective_id=0, has_side_effects=True, vmem_limit_bytes=60000000
        ),
    )(
        pressure.reshape(cells, nz),
        depth.reshape(cells, nz),
        saturation.reshape(2 * cells, nz),
        permeability.reshape(3 * cells, nz),
        pore_volume.reshape(cells, nz),
        pairs.T,
        kind,
        count,
        table,
    )
    _, _, out = pl.pallas_call(
        functools.partial(finish, cells, nz),
        out_shape=(
            pltpu.VMEM((3 * cells, nz), f32),
            pltpu.VMEM((9, CAP, 3 * nz), f32),
            jax.ShapeDtypeStruct((3 * cells, nz), f32),
        ),
        in_specs=[vmem, vmem, smem],
        out_specs=(vmem, vmem, any_spec),
        scratch_shapes=[dma],
        input_output_aliases={0: 0, 1: 1},
    )(part, res, own)
    return out.reshape(3, cx, cy, nz)


def solution(mesh):
    cell = P("gx", "gy", None)
    cells = P(None, "gx", "gy", None)
    both = ("gx", "gy")
    return jax.shard_map(
        body,
        mesh=mesh,
        in_specs=(cell, cell, cells, cells, cell, P(both, None), P(both), P(both), P()),
        out_specs=cells,
        check_vma=False,
    )
```

```python
import functools

import jax
import jax.numpy as jnp
from jax import lax
from jax.experimental import pallas as pl
from jax.experimental.pallas import tpu as pltpu
from jax.sharding import PartitionSpec as P

CAP = 4
ROWS = 2 * CAP
VISCOSITY = (0.5, 1.0, 0.25)
DENSITY = (1.0, 0.8, 0.25)
STEP = 0.2
MESH = pl.DeviceIdType.MESH
NEAR = [(dx, dy) for dx in (-1, 0, 1) for dy in ((-1, 1, 0) if dx == 0 else (-1, 0, 1))]
HOME = 5
OTHERS = [n for n in range(9) if n != HOME]
PIECES = 12


def mobility(w, o):
    g = 1.0 - w - o
    return (w * w * (1.0 / VISCOSITY[0]), o * o, g * g * (1.0 / VISCOSITY[2]))


def harmonic(a, b):
    return 2.0 * a * b / (a + b)


def flux(dp, dd, low, high, trans):
    flows = []
    for f in range(3):
        drive = dp - DENSITY[f] * dd if DENSITY[f] != 1.0 else dp - dd
        flows.append(trans * jnp.where(drive > 0.0, low[f], high[f]) * drive)
    return flows


def edge_flux(low, high):
    return flux(
        low[0] - high[0],
        low[1] - high[1],
        mobility(low[2], low[3]),
        mobility(high[2], high[3]),
        harmonic(low[4], high[4]),
    )


def kernel(
    cx, cy, nz, nrow,
    p_hbm, d_hbm, s_hbm, k_hbm, v_hbm, pairs_hbm, kind_hbm, count_hbm, table_hbm,
    out, res, own_s,
    cell, k, v, table, pairs_v, count_s, kindrow,
    idx_send, idx_s, send, recv, loc, tloc, back, ret, scl,
    xhalo, yhalo,
    ir_sem, fr_sem, br_sem, xr_sem, yr_sem,
    between, via_i, via_f, vi_sem, vf_sem, go_sem, here_sem, near_sem,
):
    def arrived(ref, sem):
        pltpu.make_async_copy(ref, ref, sem).wait()

    def seat(n):
        return n - 1 if isinstance(n, int) and n > HOME else n

    def work(load_sem, own_sem, out_sem, ws_sem, xs_sem, ys_sem):
        nx = lax.axis_size("gx")
        ny = lax.axis_size("gy")
        ix = lax.axis_index("gx")
        iy = lax.axis_index("gy")
        cells = cx * cy
        p, d, s = (cell.at[pl.ds(i * cells, (1, 1, 2)[i] * cells)] for i in range(3))

        def device(dx, dy):
            return (lax.rem(ix + dx + nx, nx), lax.rem(iy + dy + ny, ny))

        def remote(src, dst, ss, rs, dev):
            return pltpu.make_async_remote_copy(
                src_ref=src, dst_ref=dst, send_sem=ss, recv_sem=rs, device_id=dev, device_id_type=MESH
            )

        def signal(sem, dev):
            pl.semaphore_signal(sem, inc=1, device_id=dev, device_id_type=MESH)

        def wrap(y):
            return lax.rem(y + 2 * ny, ny)

        first, last = ix == 0, ix == nx - 1
        y_odd = lax.rem(iy, 2)
        relays = (ix == 1) & (y_odd == 1)
        barrier = pltpu.get_barrier_semaphore()
        for n in OTHERS:
            dx, dy = NEAR[n]
            if dx == 1:
                @pl.when(ix < nx - 2)
                def _():
                    signal(barrier, device(dx, dy))
            elif dx == 0:
                @pl.when(~first & ~last)
                def _():
                    signal(barrier, device(dx, dy))
            else:
                @pl.when((ix > 1) | relays)
                def _():
                    signal(barrier, device(dx, dy))

        @pl.when(first & (y_odd == 1))
        def _():
            signal(barrier, (1, wrap(iy + 2)))

        @pl.when(relays)
        def _():
            signal(barrier, (nx - 1, wrap(iy - 1)))
            signal(barrier, (nx - 1, iy))
            signal(barrier, (0, wrap(iy - 2)))

        @pl.when(last)
        def _():
            pl.semaphore_wait(barrier, 1)
            signal(go_sem.at[y_odd], (1, iy + 1 - y_odd))

        loads = [
            pltpu.make_async_copy(src, dst, load_sem.at[i])
            for i, src, dst in (
                (0, pairs_hbm, pairs_v),
                (1, kind_hbm, kindrow),
                (2, count_hbm, count_s),
                (3, p_hbm, p),
                (3, d_hbm, d),
                (3, s_hbm, s),
                (4, k_hbm, k),
                (5, v_hbm, v),
                (6, table_hbm, table),
            )
        ]
        for c in loads:
            c.start()

        for c in loads[:3]:
            c.wait()
        lane_of_row = lax.broadcasted_iota(jnp.int32, (nrow, nrow), 1)
        sub_of_row = lax.broadcasted_iota(jnp.int32, (nrow, nrow), 0)
        eye = lane_of_row == sub_of_row
        pv = pairs_v[...]
        tgt_row = pv[1:2, :]

        def to_sublanes(row):
            return jnp.sum(jnp.where(eye, row, 0), axis=1, keepdims=True)

        src_col = to_sublanes(pv[0:1, :])
        tgt_col = to_sublanes(tgt_row)
        land_col = to_sublanes(pv[2:3, :])
        kind_col = to_sublanes(kindrow[...].reshape(1, nrow))
        rank_col = jnp.sum(
            ((tgt_col == tgt_row) & (lane_of_row < sub_of_row)).astype(jnp.int32), axis=1, keepdims=True
        )
        live_col = (lax.broadcasted_iota(jnp.int32, (nrow, 1), 0) < count_s[0]).astype(jnp.int32)
        code_col = jnp.zeros_like(tgt_col)
        for n in range(9):
            hx, hy = device(*NEAR[n])
            code_col = jnp.where(tgt_col == hx * ny + hy, n, code_col)
        lanes = lax.broadcasted_iota(jnp.int32, (nrow, 128), 1)
        message = (
            jnp.where(lanes == rank_col, land_col, 0)
            + jnp.where(lanes == CAP + rank_col, kind_col, 0)
            + jnp.where(lanes == 2 * CAP + rank_col, live_col, 0)
            + jnp.where(lanes == 3 * CAP + rank_col, src_col, 0)
        )
        for n in range(9):
            idx_send[n] = jnp.sum(jnp.where(code_col == n, message, 0), axis=0, keepdims=True)

        own_copy = pltpu.make_async_copy(idx_send, own_s, own_sem)
        own_copy.start()
        arrived(cell, load_sem.at[3])
        own_copy.wait()
        for n in range(9):
            dst = recv if n == HOME else send
            for r in range(CAP):
                col = own_s[n, 0, 3 * CAP + r]
                dst[n, r : r + 1, :nz] = p[pl.ds(col, 1), :]
                dst[n, CAP + r : CAP + r + 1, :nz] = d[pl.ds(col, 1), :]
                dst[n, r : r + 1, nz:] = s[pl.ds(col, 1), :]
                dst[n, CAP + r : CAP + r + 1, nz:] = s[pl.ds(cells + col, 1), :]

        odd = lax.rem(ix, 2)
        away = 2 * odd - 1

        def place(dx, dy):
            if isinstance(dx, int) and dx == 0:
                return NEAR.index((0, dy))
            return 3 * (dx + 1) + dy + 1

        def ask(dx, dy):
            n = place(dx, dy)
            dev = device(dx, dy)
            slot = inbox(dx, dy)
            remote(idx_send.at[n], idx_s.at[n], out_sem, ir_sem.at[slot], dev).start()
            remote(send.at[n], recv.at[n], out_sem, fr_sem.at[slot], dev).start()

        def inbox(dx, dy):
            if isinstance(dx, int):
                return dy + 1 if dx < 0 else 3 + dx
            return jnp.where(dx < 0, dy + 1, 3 + dx)

        def relay_slot(j, off):
            if isinstance(off, int):
                return (0, 1 + j, 3 + j, 5)[off + 2]
            return jnp.where(off == -2, 0, jnp.where(off == -1, 1 + j, jnp.where(off == 0, 3 + j, 5)))

        def far_asks():
            for dy in (-1, 1, 0):
                ask(away, dy)

        def near_asks():
            for dy in (-1, 1, 0):
                ask(-away, dy)
            for dy in (-1, 1):
                ask(0, dy)

        @pl.when(first)
        def _():
            pl.semaphore_wait(barrier, 2)
            for dy in (y_odd, 1 - 2 * y_odd, y_odd - 1):
                ty = wrap(iy + dy)
                t_odd = lax.rem(ty, 2)
                off = t_odd - 1 - dy
                slot = relay_slot(t_odd, off)
                via = (1, ty + 1 - t_odd)
                remote(idx_send.at[dy + 1], via_i.at[slot], out_sem, vi_sem.at[off + 2], via).start()
                remote(send.at[dy + 1], via_f.at[slot], out_sem, vf_sem.at[off + 2], via).start()

        @pl.when(~first)
        def _():
            @pl.when(~last)
            def _():
                pl.semaphore_wait(barrier, 8 + relays.astype(jnp.int32))

            @pl.when(relays)
            def _():
                signal(barrier, (nx - 1, wrap(iy - 1)))
                signal(barrier, (nx - 1, iy))
                for off in (-2, -1, 0, 1):
                    signal(near_sem, (0, wrap(iy + off)))

            @pl.when(ix == nx - 2)
            def _():
                for dy in (-1, 0, 1):
                    signal(here_sem, device(1, dy))

            @pl.when(last)
            def _():
                pl.semaphore_wait(barrier, 1)
                for dy in (-1, 0, 1):
                    signal(here_sem, device(1, dy))
                pl.semaphore_wait(here_sem, 3)

            @pl.when(ix != 2)
            def _():
                far_asks()

        @pl.when(~first & (ix != 2))
        def _():
            near_asks()

        for c in loads[6:]:
            c.wait()
        xparts = [(p, 0), (d, 0), (s, 0), (s, cells), (k, 0)]
        yparts = [(p, 0), (d, 0), (s, 0), (s, cx), (k, cx)]

        def xcopy(side, f):
            ref, base = xparts[f]
            at = base + (0 if side == 0 else cells - cy)
            return remote(
                ref.at[pl.ds(at, cy), :], xhalo.at[1 - side, f], xs_sem.at[side], xr_sem.at[1 - side],
                device(-1 if side == 0 else 1, 0),
            )

        for f in range(5):
            ref, base = yparts[f]
            base = base * cy if f >= 3 else base
            for side in range(2):
                off = base + (0 if side == 0 else cy - 1)
                yhalo[2 + side, f] = ref[pl.ds(off, cx, stride=cy), :]

        def ycopy(side):
            return remote(
                yhalo.at[2 + side], yhalo.at[1 - side], ys_sem.at[side], yr_sem.at[1 - side],
                device(0, -1 if side == 0 else 1),
            )

        zmask = lax.broadcasted_iota(jnp.int32, (cy, nz), 1) < nz - 1
        ymask = lax.broadcasted_iota(jnp.int32, (cy, nz), 0) < cy - 1

        def slab(a, carry):
            base = pl.multiple_of(a * cy, cy)
            after = pl.multiple_of(jnp.minimum(a + 1, cx - 1) * cy, cy)

            def at(ref, off):
                return ref[pl.ds(off, cy), :]

            p0, d0 = at(p, base), at(d, base)
            w0, o0 = at(s, base), at(s, cells + base)
            m0 = mobility(w0, o0)
            m1 = mobility(at(s, after), at(s, cells + after))
            tx = jnp.where(a < cx - 1, harmonic(at(k, base), at(k, after)), 0.0)
            fx = flux(p0 - at(p, after), d0 - at(d, after), m0, m1, tx)
            net = [fx[f] - carry[f] for f in range(3)]
            for axis, size, mask, offset in ((0, cy, ymask, cells), (1, nz, zmask, 2 * cells)):
                def up(x):
                    return pltpu.roll(x, size - 1, axis)

                kk = at(k, offset + base)
                t = jnp.where(mask, harmonic(kk, up(kk)), 0.0)
                fl = flux(p0 - up(p0), d0 - up(d0), m0, [up(m) for m in m0], t)
                net = [net[f] + (fl[f] - pltpu.roll(fl[f], 1, axis)) for f in range(3)]
            scale = STEP / at(v, base)
            v[pl.ds(base, cy), :] = scale
            now = (w0, o0, 1.0 - w0 - o0)
            for f in range(3):
                out[pl.ds(f * cells + base, cy), :] = now[f] - scale * net[f]
            return tuple(fx)

        zero = jnp.zeros((cy, nz), jnp.float32)
        quarter = cx // 4

        def march(start, stop):
            before = tuple(between[f] for f in range(3)) if start else (zero, zero, zero)
            edge = lax.fori_loop(start, stop, slab, before, unroll=2)
            if stop < cx:
                for f in range(3):
                    between[f] = edge[f]

        march(0, quarter)

        @pl.when(ix == 2)
        def _():
            far_asks()

        @pl.when(first)
        def _():
            pl.semaphore_wait(near_sem, 2)

        @pl.when(first | (ix == 2))
        def _():
            near_asks()

        def take(off):
            start, many = ((0, 1), (1, 2), (3, 2), (5, 1))[off + 2]
            arrived(via_i.at[pl.ds(start, many)], vi_sem.at[off + 2])
            arrived(via_f.at[pl.ds(start, many)], vf_sem.at[off + 2])

        def onward(j, off):
            dy = j - 1 - off
            slot, dev = relay_slot(j, off), (nx - 1, wrap(iy - 1 + j))
            remote(via_i.at[slot], idx_s.at[dy + 1], ws_sem, ir_sem.at[dy + 1], dev).start()
            remote(via_f.at[slot], recv.at[dy + 1], ws_sem, fr_sem.at[dy + 1], dev).start()

        def pass_on(plan):
            for step in plan:
                if step in ("even", "odd"):
                    pl.semaphore_wait(go_sem.at[int(step == "odd")], 1)
                elif isinstance(step, int):
                    take(step)
                else:
                    onward(*step)

        @pl.when(relays & (iy == 1))
        def _():
            pass_on(["odd", "even", 0, (0, 0), (1, 0), -1, (0, -1), (1, -1), -2, (0, -2), 1, (1, 1)])

        @pl.when(relays & (iy != 1))
        def _():
            pass_on(["even", -2, (0, -2), "odd", 1, (1, 1), 0, (0, 0), (1, 0), -1, (0, -1), (1, -1)])

        march(quarter, 2 * quarter)
        has = ((ix > 0, ix < nx - 1), (iy > 0, iy < ny - 1))
        for side in range(2):
            @pl.when(has[0][side])
            def _():
                for f in range(5):
                    xcopy(side, f).start()

            @pl.when(has[1][side])
            def _():
                ycopy(side).start()

        @pl.when(~last)
        def _():
            march(2 * quarter, cx)

        def answer(n, ints):
            for r in range(CAP):
                land = ints[n, 0, r]
                kd = ints[n, 0, CAP + r]
                live = ints[n, 0, 2 * CAP + r].astype(jnp.float32)
                loc[n, r : r + 1, :nz] = p[pl.ds(land, 1), :]
                loc[n, CAP + r : CAP + r + 1, :nz] = d[pl.ds(land, 1), :]
                loc[n, r : r + 1, nz:] = s[pl.ds(land, 1), :]
                loc[n, CAP + r : CAP + r + 1, nz:] = s[pl.ds(cells + land, 1), :]
                tloc[n, r : r + 1, :] = table[pl.ds(kd, 1), :] * live

        def flows_of(start, many):
            rows = pl.ds(start, many)
            far, here = recv[rows], loc[rows]

            def second(x):
                return pltpu.roll(x, CAP, 1)

            gap = far[:, :, :nz] - here[:, :, :nz]
            fl = flux(
                gap,
                second(gap),
                mobility(far[:, :, nz:], second(far[:, :, nz:])),
                mobility(here[:, :, nz:], second(here[:, :, nz:])),
                tloc[rows],
            )
            for f in range(3):
                back[rows, :, f * nz : (f + 1) * nz] = fl[f][:, :CAP]

        def reply(dx, dy):
            n = place(dx, dy)
            return remote(back.at[n], ret.at[seat(n)], out_sem, br_sem, device(-dx, -dy))

        def landed(buf, sem, dx):
            start = 3 * (dx + 1)
            if dx < 0:
                for i in range(3):
                    arrived(buf.at[i], sem.at[i])
            else:
                arrived(buf.at[pl.ds(start, 2 + dx)], sem.at[3 + dx])

        def serve(dx):
            start = 3 * (dx + 1)
            landed(idx_s, ir_sem, dx)
            for i in range(3):
                answer(start + i, own_s if start + i == HOME else idx_s)
            landed(recv, fr_sem, dx)
            flows_of(start, 3)
            if dx == 1:
                @pl.when(first)
                def _():
                    pl.semaphore_wait(here_sem, 3)

            for dy in (-1, 1, 0):
                if dx or dy:
                    reply(dx, dy).start()

        @pl.when(last)
        def _():
            side = jnp.where((iy == 0) | (iy == ny - 1), -1, 1)
            for dy in (side, 0, -side):
                n = dy + 1
                arrived(idx_s.at[n], ir_sem.at[n])
                answer(n, idx_s)
                arrived(recv.at[n], fr_sem.at[n])
                flows_of(n, 1)
                reply(-1, dy).start()

        serve(0)

        @pl.when(odd == 1)
        def _():
            serve(1)

        @pl.when(~last)
        def _():
            serve(-1)

        @pl.when(odd == 0)
        def _():
            serve(1)

        @pl.when(last)
        def _():
            march(2 * quarter, cx)

        for side in range(2):
            @pl.when(has[0][side])
            def _():
                arrived(xhalo.at[side], xs_sem.at[side])
                arrived(xhalo.at[side], xr_sem.at[side])
                at = 0 if side == 0 else cells - cy
                mine = [ref[pl.ds(base + at, cy), :] for ref, base in xparts]
                near = [xhalo[side, f] for f in range(5)]
                low, high = (near, mine) if side == 0 else (mine, near)
                fl = edge_flux(low, high)
                scale = v[pl.ds(at, cy), :]
                for f in range(3):
                    rows = pl.ds(f * cells + at, cy)
                    out[rows, :] = out[rows, :] + (scale * fl[f] if side == 0 else -scale * fl[f])

        for side in range(2):
            @pl.when(has[1][side])
            def _():
                ycopy(side).wait_send()
                ycopy(1 - side).wait_recv()
                at = 0 if side == 0 else cy - 1
                mine = [yhalo[2 + side, f] for f in range(5)]
                near = [yhalo[side, f] for f in range(5)]
                low, high = (near, mine) if side == 0 else (mine, near)
                fl = edge_flux(low, high)
                scale = v[pl.ds(at, cx, stride=cy), :]
                for f in range(3):
                    rows = pl.ds(f * cells + at, cx, stride=cy)
                    out[rows, :] = out[rows, :] + (scale * fl[f] if side == 0 else -scale * fl[f])

        lane1 = lax.broadcasted_iota(jnp.int32, (1, 128), 1)
        slots = 10 * CAP
        spot = jnp.full((1, 128), -1, jnp.int32)
        for n in range(9):
            for r in range(CAP):
                spot = jnp.where(lane1 == n * CAP + r, (own_s if n == HOME else idx_s)[n, 0, r], spot)
        for r in range(CAP):
            spot = jnp.where(lane1 == 9 * CAP + r, own_s[HOME, 0, 3 * CAP + r], spot)
        spot = jnp.where(lane1 < slots, spot, 0)
        spot = spot + pltpu.roll(spot, slots, 1) + pltpu.roll(spot, 2 * slots, 1)
        flows = jnp.concatenate([-back[n] for n in range(9)] + [back[HOME]], axis=0)
        hi = flows.astype(jnp.bfloat16).astype(jnp.float32)
        rest = flows - hi
        mid = rest.astype(jnp.bfloat16).astype(jnp.float32)
        pad = jnp.zeros((128 - 3 * slots, 3 * nz), jnp.float32)
        parts = jnp.concatenate([hi, mid, rest - mid, pad], axis=0).astype(jnp.bfloat16)
        step = 8 * cy
        for c in range(cells // step):
            ids = lax.broadcasted_iota(jnp.int32, (step, 128), 0) + c * step
            hot = (ids == spot).astype(jnp.float32).astype(jnp.bfloat16)
            add = jnp.dot(hot, parts, preferred_element_type=jnp.float32)
            scale = v[c * step : (c + 1) * step, :]
            for f in range(3):
                at = pl.ds(f * cells + c * step, step)
                out[at, :] = out[at, :] - scale * add[:, f * nz : (f + 1) * nz]

        for n in OTHERS:
            for r in range(CAP):
                scl[n, r : r + 1, :] = v[pl.ds(own_s[n, 0, 3 * CAP + r], 1), :]
        @pl.when(relays)
        def _():
            arrived(cell.at[pl.ds(0, 6 * (1 + 2 * ROWS))], ws_sem)

        arrived(cell.at[pl.ds(0, 8 * (1 + 2 * ROWS + 3 * CAP))], out_sem)
    dma = pltpu.SemaphoreType.DMA
    pl.run_scoped(work, dma((7,)), dma, dma, dma, dma((2,)), dma((2,)))
    arrived(ret, br_sem)
    for n in OTHERS:
        for f in range(3):
            res[n, :, f * nz : (f + 1) * nz] = ret[seat(n), :, f * nz : (f + 1) * nz] * scl[n]


def finish(cells, nz, part, res_in, own_s, held, res, final, sem):
    for n in OTHERS:
        for r in range(CAP):
            col = own_s[n, 0, 3 * CAP + r]
            for f in range(3):
                row = pl.ds(f * cells + col, 1)
                held[row, :] = held[row, :] - res[n, r : r + 1, f * nz : (f + 1) * nz]
    size = 3 * cells // PIECES
    for i in range(PIECES):
        rows = pl.ds(i * size, size)
        pltpu.make_async_copy(held.at[rows], final.at[rows], sem).start()
    pltpu.make_async_copy(held, final, sem).wait()


def body(pressure, depth, saturation, permeability, pore_volume, pairs, kind, count, table):
    cx, cy, nz = pressure.shape
    nrow = pairs.shape[0]
    kinds = table.shape[0]
    cells = cx * cy
    f32 = jnp.float32
    dma = pltpu.SemaphoreType.DMA
    regular = pltpu.SemaphoreType.REGULAR
    any_spec = pl.BlockSpec(memory_space=pltpu.HBM)
    vmem = pl.BlockSpec(memory_space=pltpu.VMEM)
    smem = pl.BlockSpec(memory_space=pltpu.SMEM)
    part, res, own = pl.pallas_call(
        functools.partial(kernel, cx, cy, nz, nrow),
        out_shape=(
            pltpu.VMEM((3 * cells, nz), f32),
            pltpu.VMEM((9, CAP, 3 * nz), f32),
            pltpu.SMEM((9, 1, 128), jnp.int32),
        ),
        in_specs=[any_spec] * 9,
        out_specs=(vmem, vmem, smem),
        scratch_shapes=[
            pltpu.VMEM((4 * cells, nz), f32),
            pltpu.VMEM((3 * cells, nz), f32),
            pltpu.VMEM((cells, nz), f32),
            pltpu.VMEM((kinds, nz), f32),
            pltpu.VMEM((3, nrow), jnp.int32),
            pltpu.SMEM((1,), jnp.int32),
            pltpu.VMEM((nrow,), jnp.int32),
            pltpu.VMEM((9, 1, 128), jnp.int32),
            pltpu.SMEM((9, 1, 128), jnp.int32),
            pltpu.VMEM((9, ROWS, 2 * nz), f32),
            pltpu.VMEM((9, ROWS, 2 * nz), f32),
            pltpu.VMEM((9, ROWS, 2 * nz), f32),
            pltpu.VMEM((9, ROWS, nz), f32),
            pltpu.VMEM((9, CAP, 3 * nz), f32),
            pltpu.VMEM((8, CAP, 3 * nz), f32),
            pltpu.VMEM((9, CAP, nz), f32),
            pltpu.VMEM((2, 5, cy, nz), f32),
            pltpu.VMEM((4, 5, cx, nz), f32),
            dma((5,)), dma((5,)), dma, dma((2,)), dma((2,)),
            pltpu.VMEM((3, cy, nz), f32),
            pltpu.VMEM((6, 1, 128), jnp.int32),
            pltpu.VMEM((6, ROWS, 2 * nz), f32),
            dma((4,)), dma((4,)), regular((2,)), regular, regular,
        ],
        compiler_params=pltpu.CompilerParams(
            collective_id=0, has_side_effects=True, vmem_limit_bytes=60000000
        ),
    )(
        pressure.reshape(cells, nz),
        depth.reshape(cells, nz),
        saturation.reshape(2 * cells, nz),
        permeability.reshape(3 * cells, nz),
        pore_volume.reshape(cells, nz),
        pairs.T,
        kind,
        count,
        table,
    )
    _, _, out = pl.pallas_call(
        functools.partial(finish, cells, nz),
        out_shape=(
            pltpu.VMEM((3 * cells, nz), f32),
            pltpu.VMEM((9, CAP, 3 * nz), f32),
            jax.ShapeDtypeStruct((3 * cells, nz), f32),
        ),
        in_specs=[vmem, vmem, smem],
        out_specs=(vmem, vmem, any_spec),
        scratch_shapes=[dma],
        input_output_aliases={0: 0, 1: 1},
    )(part, res, own)
    return out.reshape(3, cx, cy, nz)


def solution(mesh):
    cell = P("gx", "gy", None)
    cells = P(None, "gx", "gy", None)
    both = ("gx", "gy")
    return jax.shard_map(
        body,
        mesh=mesh,
        in_specs=(cell, cell, cells, cells, cell, P(both, None), P(both), P(both), P()),
        out_specs=cells,
        check_vma=False,
    )
```

```python
import functools

import jax
import jax.numpy as jnp
from jax import lax
from jax.experimental import pallas as pl
from jax.experimental.pallas import tpu as pltpu
from jax.sharding import PartitionSpec as P

CAP = 4
ROWS = 2 * CAP
VISCOSITY = (0.5, 1.0, 0.25)
DENSITY = (1.0, 0.8, 0.25)
STEP = 0.2
MESH = pl.DeviceIdType.MESH
NEAR = [(dx, dy) for dx in (-1, 0, 1) for dy in ((-1, 1, 0) if dx == 0 else (-1, 0, 1))]
HOME = 5
OTHERS = [n for n in range(9) if n != HOME]
PIECES = 12


def mobility(w, o):
    g = 1.0 - w - o
    return (w * w * (1.0 / VISCOSITY[0]), o * o, g * g * (1.0 / VISCOSITY[2]))


def harmonic(a, b):
    return 2.0 * a * b / (a + b)


def flux(dp, dd, low, high, trans):
    flows = []
    for f in range(3):
        drive = dp - DENSITY[f] * dd if DENSITY[f] != 1.0 else dp - dd
        flows.append(trans * jnp.where(drive > 0.0, low[f], high[f]) * drive)
    return flows


def edge_flux(low, high):
    return flux(
        low[0] - high[0],
        low[1] - high[1],
        mobility(low[2], low[3]),
        mobility(high[2], high[3]),
        harmonic(low[4], high[4]),
    )


def kernel(
    cx, cy, nz, nrow,
    p_hbm, d_hbm, s_hbm, k_hbm, v_hbm, pairs_hbm, kind_hbm, count_hbm, table_hbm,
    out, res, own_s,
    cell, k, v, table, pairs_v, count_s, kindrow,
    idx_send, idx_s, send, recv, loc, tloc, back, ret, scl,
    xhalo, yhalo,
    ir_sem, fr_sem, br_sem, xr_sem, yr_sem,
    between, via_i, via_f, vi_sem, vf_sem, go_sem, here_sem, near_sem,
):
    def arrived(ref, sem):
        pltpu.make_async_copy(ref, ref, sem).wait()

    def seat(n):
        return n - 1 if isinstance(n, int) and n > HOME else n

    def work(load_sem, own_sem, out_sem, ws_sem, xs_sem, ys_sem):
        nx = lax.axis_size("gx")
        ny = lax.axis_size("gy")
        ix = lax.axis_index("gx")
        iy = lax.axis_index("gy")
        cells = cx * cy
        p, d, s = (cell.at[pl.ds(i * cells, (1, 1, 2)[i] * cells)] for i in range(3))

        def device(dx, dy):
            return (lax.rem(ix + dx + nx, nx), lax.rem(iy + dy + ny, ny))

        def remote(src, dst, ss, rs, dev):
            return pltpu.make_async_remote_copy(
                src_ref=src, dst_ref=dst, send_sem=ss, recv_sem=rs, device_id=dev, device_id_type=MESH
            )

        def signal(sem, dev):
            pl.semaphore_signal(sem, inc=1, device_id=dev, device_id_type=MESH)

        def wrap(y):
            return lax.rem(y + 2 * ny, ny)

        first, last = ix == 0, ix == nx - 1
        y_odd = lax.rem(iy, 2)
        relays = (ix == 1) & (y_odd == 1)
        barrier = pltpu.get_barrier_semaphore()
        @pl.when(relays)
        def _():
            signal(barrier, (nx - 1, wrap(iy - 1)))
            signal(barrier, (nx - 1, iy))
            signal(barrier, (0, wrap(iy - 2)))

        @pl.when(last)
        def _():
            pl.semaphore_wait(barrier, 1)
            signal(go_sem.at[y_odd], (1, iy + 1 - y_odd))

        for n in OTHERS:
            dx, dy = NEAR[n]
            if dx == 1:
                @pl.when(ix < nx - 2)
                def _():
                    signal(barrier, device(dx, dy))
            elif dx == 0:
                @pl.when(~first & ~last)
                def _():
                    signal(barrier, device(dx, dy))
            else:
                @pl.when((ix > 1) | relays)
                def _():
                    signal(barrier, device(dx, dy))

        @pl.when(first & (y_odd == 1))
        def _():
            signal(barrier, (1, wrap(iy + 2)))

        loads = [
            pltpu.make_async_copy(src, dst, load_sem.at[i])
            for i, src, dst in (
                (0, pairs_hbm, pairs_v),
                (1, kind_hbm, kindrow),
                (2, count_hbm, count_s),
                (3, p_hbm, p),
                (3, d_hbm, d),
                (3, s_hbm, s),
                (4, k_hbm, k),
                (5, v_hbm, v),
                (6, table_hbm, table),
            )
        ]
        for c in loads:
            c.start()

        for c in loads[:3]:
            c.wait()
        lane_of_row = lax.broadcasted_iota(jnp.int32, (nrow, nrow), 1)
        sub_of_row = lax.broadcasted_iota(jnp.int32, (nrow, nrow), 0)
        eye = lane_of_row == sub_of_row
        pv = pairs_v[...]
        tgt_row = pv[1:2, :]

        def to_sublanes(row):
            return jnp.sum(jnp.where(eye, row, 0), axis=1, keepdims=True)

        src_col = to_sublanes(pv[0:1, :])
        tgt_col = to_sublanes(tgt_row)
        land_col = to_sublanes(pv[2:3, :])
        kind_col = to_sublanes(kindrow[...].reshape(1, nrow))
        rank_col = jnp.sum(
            ((tgt_col == tgt_row) & (lane_of_row < sub_of_row)).astype(jnp.int32), axis=1, keepdims=True
        )
        live_col = (lax.broadcasted_iota(jnp.int32, (nrow, 1), 0) < count_s[0]).astype(jnp.int32)
        code_col = jnp.zeros_like(tgt_col)
        for n in range(9):
            hx, hy = device(*NEAR[n])
            code_col = jnp.where(tgt_col == hx * ny + hy, n, code_col)
        lanes = lax.broadcasted_iota(jnp.int32, (nrow, 128), 1)
        message = (
            jnp.where(lanes == rank_col, land_col, 0)
            + jnp.where(lanes == CAP + rank_col, kind_col, 0)
            + jnp.where(lanes == 2 * CAP + rank_col, live_col, 0)
            + jnp.where(lanes == 3 * CAP + rank_col, src_col, 0)
        )
        for n in range(9):
            idx_send[n] = jnp.sum(jnp.where(code_col == n, message, 0), axis=0, keepdims=True)

        own_copy = pltpu.make_async_copy(idx_send, own_s, own_sem)
        own_copy.start()
        arrived(cell, load_sem.at[3])
        own_copy.wait()
        for n in range(9):
            dst = recv if n == HOME else send
            for r in range(CAP):
                col = own_s[n, 0, 3 * CAP + r]
                dst[n, r : r + 1, :nz] = p[pl.ds(col, 1), :]
                dst[n, CAP + r : CAP + r + 1, :nz] = d[pl.ds(col, 1), :]
                dst[n, r : r + 1, nz:] = s[pl.ds(col, 1), :]
                dst[n, CAP + r : CAP + r + 1, nz:] = s[pl.ds(cells + col, 1), :]

        odd = lax.rem(ix, 2)
        away = 2 * odd - 1

        def place(dx, dy):
            if isinstance(dx, int) and dx == 0:
                return NEAR.index((0, dy))
            return 3 * (dx + 1) + dy + 1

        def ask(dx, dy):
            n = place(dx, dy)
            dev = device(dx, dy)
            slot = inbox(dx, dy)
            remote(idx_send.at[n], idx_s.at[n], out_sem, ir_sem.at[slot], dev).start()
            remote(send.at[n], recv.at[n], out_sem, fr_sem.at[slot], dev).start()

        def inbox(dx, dy):
            if isinstance(dx, int):
                return dy + 1 if dx < 0 else 3 + dx
            return jnp.where(dx < 0, dy + 1, 3 + dx)

        def relay_slot(j, off):
            if isinstance(off, int):
                return (0, 1 + j, 3 + j, 5)[off + 2]
            return jnp.where(off == -2, 0, jnp.where(off == -1, 1 + j, jnp.where(off == 0, 3 + j, 5)))

        def far_asks():
            for dy in (-1, 1, 0):
                ask(away, dy)

        def near_asks():
            for dy in (-1, 1, 0):
                ask(-away, dy)
            for dy in (-1, 1):
                ask(0, dy)

        @pl.when(first)
        def _():
            pl.semaphore_wait(barrier, 2)
            for dy in (y_odd, 1 - 2 * y_odd, y_odd - 1):
                ty = wrap(iy + dy)
                t_odd = lax.rem(ty, 2)
                off = t_odd - 1 - dy
                slot = relay_slot(t_odd, off)
                via = (1, ty + 1 - t_odd)
                remote(idx_send.at[dy + 1], via_i.at[slot], out_sem, vi_sem.at[off + 2], via).start()
                remote(send.at[dy + 1], via_f.at[slot], out_sem, vf_sem.at[off + 2], via).start()

        @pl.when(~first)
        def _():
            @pl.when(~last)
            def _():
                pl.semaphore_wait(barrier, 8 + relays.astype(jnp.int32))

            @pl.when(relays)
            def _():
                signal(barrier, (nx - 1, wrap(iy - 1)))
                signal(barrier, (nx - 1, iy))
                for off in (-2, -1, 0, 1):
                    signal(near_sem, (0, wrap(iy + off)))

            @pl.when(ix == nx - 2)
            def _():
                for dy in (-1, 0, 1):
                    signal(here_sem, device(1, dy))

            @pl.when(last)
            def _():
                pl.semaphore_wait(barrier, 1)
                for dy in (-1, 0, 1):
                    signal(here_sem, device(1, dy))
                pl.semaphore_wait(here_sem, 3)

            @pl.when(ix != 2)
            def _():
                far_asks()

        @pl.when(~first & (ix != 2))
        def _():
            near_asks()

        for c in loads[6:]:
            c.wait()
        xparts = [(p, 0), (d, 0), (s, 0), (s, cells), (k, 0)]
        yparts = [(p, 0), (d, 0), (s, 0), (s, cx), (k, cx)]

        def xcopy(side, f):
            ref, base = xparts[f]
            at = base + (0 if side == 0 else cells - cy)
            return remote(
                ref.at[pl.ds(at, cy), :], xhalo.at[1 - side, f], xs_sem.at[side], xr_sem.at[1 - side],
                device(-1 if side == 0 else 1, 0),
            )

        for f in range(5):
            ref, base = yparts[f]
            base = base * cy if f >= 3 else base
            for side in range(2):
                off = base + (0 if side == 0 else cy - 1)
                yhalo[2 + side, f] = ref[pl.ds(off, cx, stride=cy), :]

        def ycopy(side):
            return remote(
                yhalo.at[2 + side], yhalo.at[1 - side], ys_sem.at[side], yr_sem.at[1 - side],
                device(0, -1 if side == 0 else 1),
            )

        zmask = lax.broadcasted_iota(jnp.int32, (cy, nz), 1) < nz - 1
        ymask = lax.broadcasted_iota(jnp.int32, (cy, nz), 0) < cy - 1

        def slab(a, carry):
            base = pl.multiple_of(a * cy, cy)
            after = pl.multiple_of(jnp.minimum(a + 1, cx - 1) * cy, cy)

            def at(ref, off):
                return ref[pl.ds(off, cy), :]

            p0, d0 = at(p, base), at(d, base)
            w0, o0 = at(s, base), at(s, cells + base)
            m0 = mobility(w0, o0)
            m1 = mobility(at(s, after), at(s, cells + after))
            tx = jnp.where(a < cx - 1, harmonic(at(k, base), at(k, after)), 0.0)
            fx = flux(p0 - at(p, after), d0 - at(d, after), m0, m1, tx)
            net = [fx[f] - carry[f] for f in range(3)]
            for axis, size, mask, offset in ((0, cy, ymask, cells), (1, nz, zmask, 2 * cells)):
                def up(x):
                    return pltpu.roll(x, size - 1, axis)

                kk = at(k, offset + base)
                t = jnp.where(mask, harmonic(kk, up(kk)), 0.0)
                fl = flux(p0 - up(p0), d0 - up(d0), m0, [up(m) for m in m0], t)
                net = [net[f] + (fl[f] - pltpu.roll(fl[f], 1, axis)) for f in range(3)]
            scale = STEP / at(v, base)
            v[pl.ds(base, cy), :] = scale
            now = (w0, o0, 1.0 - w0 - o0)
            for f in range(3):
                out[pl.ds(f * cells + base, cy), :] = now[f] - scale * net[f]
            return tuple(fx)

        zero = jnp.zeros((cy, nz), jnp.float32)
        quarter = cx // 4

        def march(start, stop):
            before = tuple(between[f] for f in range(3)) if start else (zero, zero, zero)
            edge = lax.fori_loop(start, stop, slab, before, unroll=2)
            if stop < cx:
                for f in range(3):
                    between[f] = edge[f]

        march(0, quarter)

        @pl.when(ix == 2)
        def _():
            far_asks()

        @pl.when(first)
        def _():
            pl.semaphore_wait(near_sem, 2)

        @pl.when(first | (ix == 2))
        def _():
            near_asks()

        def take(off):
            start, many = ((0, 1), (1, 2), (3, 2), (5, 1))[off + 2]
            arrived(via_i.at[pl.ds(start, many)], vi_sem.at[off + 2])
            arrived(via_f.at[pl.ds(start, many)], vf_sem.at[off + 2])

        def onward(j, off):
            dy = j - 1 - off
            slot, dev = relay_slot(j, off), (nx - 1, wrap(iy - 1 + j))
            remote(via_i.at[slot], idx_s.at[dy + 1], ws_sem, ir_sem.at[dy + 1], dev).start()
            remote(via_f.at[slot], recv.at[dy + 1], ws_sem, fr_sem.at[dy + 1], dev).start()

        def pass_on(plan):
            for step in plan:
                if step in ("even", "odd"):
                    pl.semaphore_wait(go_sem.at[int(step == "odd")], 1)
                elif isinstance(step, int):
                    take(step)
                else:
                    onward(*step)

        @pl.when(relays & (iy == 1))
        def _():
            pass_on(["odd", "even", 0, (0, 0), (1, 0), -1, (0, -1), (1, -1), -2, (0, -2), 1, (1, 1)])

        @pl.when(relays & (iy != 1))
        def _():
            pass_on(["even", -2, (0, -2), "odd", 1, (1, 1), 0, (0, 0), (1, 0), -1, (0, -1), (1, -1)])

        march(quarter, 2 * quarter)
        has = ((ix > 0, ix < nx - 1), (iy > 0, iy < ny - 1))
        for side in range(2):
            @pl.when(has[0][side])
            def _():
                for f in range(5):
                    xcopy(side, f).start()

            @pl.when(has[1][side])
            def _():
                ycopy(side).start()

        @pl.when(~last)
        def _():
            march(2 * quarter, cx)

        def answer(n, ints):
            for r in range(CAP):
                land = ints[n, 0, r]
                kd = ints[n, 0, CAP + r]
                live = ints[n, 0, 2 * CAP + r].astype(jnp.float32)
                loc[n, r : r + 1, :nz] = p[pl.ds(land, 1), :]
                loc[n, CAP + r : CAP + r + 1, :nz] = d[pl.ds(land, 1), :]
                loc[n, r : r + 1, nz:] = s[pl.ds(land, 1), :]
                loc[n, CAP + r : CAP + r + 1, nz:] = s[pl.ds(cells + land, 1), :]
                tloc[n, r : r + 1, :] = table[pl.ds(kd, 1), :] * live

        def flows_of(start, many):
            rows = pl.ds(start, many)
            far, here = recv[rows], loc[rows]

            def second(x):
                return pltpu.roll(x, CAP, 1)

            gap = far[:, :, :nz] - here[:, :, :nz]
            fl = flux(
                gap,
                second(gap),
                mobility(far[:, :, nz:], second(far[:, :, nz:])),
                mobility(here[:, :, nz:], second(here[:, :, nz:])),
                tloc[rows],
            )
            for f in range(3):
                back[rows, :, f * nz : (f + 1) * nz] = fl[f][:, :CAP]

        def reply(dx, dy):
            n = place(dx, dy)
            return remote(back.at[n], ret.at[seat(n)], out_sem, br_sem, device(-dx, -dy))

        def landed(buf, sem, dx):
            start = 3 * (dx + 1)
            if dx < 0:
                for i in range(3):
                    arrived(buf.at[i], sem.at[i])
            else:
                arrived(buf.at[pl.ds(start, 2 + dx)], sem.at[3 + dx])

        def serve(dx):
            start = 3 * (dx + 1)
            landed(idx_s, ir_sem, dx)
            for i in range(3):
                answer(start + i, own_s if start + i == HOME else idx_s)
            landed(recv, fr_sem, dx)
            flows_of(start, 3)
            if dx == 1:
                @pl.when(first)
                def _():
                    pl.semaphore_wait(here_sem, 3)

            for dy in (-1, 1, 0):
                if dx or dy:
                    reply(dx, dy).start()

        @pl.when(last)
        def _():
            side = jnp.where((iy == 0) | (iy == ny - 1), -1, 1)
            for dy in (side, 0, -side):
                n = dy + 1
                arrived(idx_s.at[n], ir_sem.at[n])
                answer(n, idx_s)
                arrived(recv.at[n], fr_sem.at[n])
                flows_of(n, 1)
                reply(-1, dy).start()

        serve(0)

        @pl.when(odd == 1)
        def _():
            serve(1)

        @pl.when(~last)
        def _():
            serve(-1)

        @pl.when(odd == 0)
        def _():
            serve(1)

        @pl.when(last)
        def _():
            march(2 * quarter, cx)

        for side in range(2):
            @pl.when(has[0][side])
            def _():
                arrived(xhalo.at[side], xs_sem.at[side])
                arrived(xhalo.at[side], xr_sem.at[side])
                at = 0 if side == 0 else cells - cy
                mine = [ref[pl.ds(base + at, cy), :] for ref, base in xparts]
                near = [xhalo[side, f] for f in range(5)]
                low, high = (near, mine) if side == 0 else (mine, near)
                fl = edge_flux(low, high)
                scale = v[pl.ds(at, cy), :]
                for f in range(3):
                    rows = pl.ds(f * cells + at, cy)
                    out[rows, :] = out[rows, :] + (scale * fl[f] if side == 0 else -scale * fl[f])

        for side in range(2):
            @pl.when(has[1][side])
            def _():
                ycopy(side).wait_send()
                ycopy(1 - side).wait_recv()
                at = 0 if side == 0 else cy - 1
                mine = [yhalo[2 + side, f] for f in range(5)]
                near = [yhalo[side, f] for f in range(5)]
                low, high = (near, mine) if side == 0 else (mine, near)
                fl = edge_flux(low, high)
                scale = v[pl.ds(at, cx, stride=cy), :]
                for f in range(3):
                    rows = pl.ds(f * cells + at, cx, stride=cy)
                    out[rows, :] = out[rows, :] + (scale * fl[f] if side == 0 else -scale * fl[f])

        lane1 = lax.broadcasted_iota(jnp.int32, (1, 128), 1)
        slots = 10 * CAP
        spot = jnp.full((1, 128), -1, jnp.int32)
        for n in range(9):
            for r in range(CAP):
                spot = jnp.where(lane1 == n * CAP + r, (own_s if n == HOME else idx_s)[n, 0, r], spot)
        for r in range(CAP):
            spot = jnp.where(lane1 == 9 * CAP + r, own_s[HOME, 0, 3 * CAP + r], spot)
        spot = jnp.where(lane1 < slots, spot, 0)
        spot = spot + pltpu.roll(spot, slots, 1) + pltpu.roll(spot, 2 * slots, 1)
        flows = jnp.concatenate([-back[n] for n in range(9)] + [back[HOME]], axis=0)
        hi = flows.astype(jnp.bfloat16).astype(jnp.float32)
        rest = flows - hi
        mid = rest.astype(jnp.bfloat16).astype(jnp.float32)
        pad = jnp.zeros((128 - 3 * slots, 3 * nz), jnp.float32)
        parts = jnp.concatenate([hi, mid, rest - mid, pad], axis=0).astype(jnp.bfloat16)
        step = 8 * cy
        for c in range(cells // step):
            ids = lax.broadcasted_iota(jnp.int32, (step, 128), 0) + c * step
            hot = (ids == spot).astype(jnp.float32).astype(jnp.bfloat16)
            add = jnp.dot(hot, parts, preferred_element_type=jnp.float32)
            scale = v[c * step : (c + 1) * step, :]
            for f in range(3):
                at = pl.ds(f * cells + c * step, step)
                out[at, :] = out[at, :] - scale * add[:, f * nz : (f + 1) * nz]

        for n in OTHERS:
            for r in range(CAP):
                scl[n, r : r + 1, :] = v[pl.ds(own_s[n, 0, 3 * CAP + r], 1), :]
        @pl.when(relays)
        def _():
            arrived(cell.at[pl.ds(0, 6 * (1 + 2 * ROWS))], ws_sem)

        arrived(cell.at[pl.ds(0, 8 * (1 + 2 * ROWS + 3 * CAP))], out_sem)
    dma = pltpu.SemaphoreType.DMA
    pl.run_scoped(work, dma((7,)), dma, dma, dma, dma((2,)), dma((2,)))
    arrived(ret, br_sem)
    for n in OTHERS:
        for f in range(3):
            res[n, :, f * nz : (f + 1) * nz] = ret[seat(n), :, f * nz : (f + 1) * nz] * scl[n]


def finish(cells, nz, part, res_in, own_s, held, res, final, sem):
    for n in OTHERS:
        for r in range(CAP):
            col = own_s[n, 0, 3 * CAP + r]
            for f in range(3):
                row = pl.ds(f * cells + col, 1)
                held[row, :] = held[row, :] - res[n, r : r + 1, f * nz : (f + 1) * nz]
    size = 3 * cells // PIECES
    for i in range(PIECES):
        rows = pl.ds(i * size, size)
        pltpu.make_async_copy(held.at[rows], final.at[rows], sem).start()
    pltpu.make_async_copy(held, final, sem).wait()


def body(pressure, depth, saturation, permeability, pore_volume, pairs, kind, count, table):
    cx, cy, nz = pressure.shape
    nrow = pairs.shape[0]
    kinds = table.shape[0]
    cells = cx * cy
    f32 = jnp.float32
    dma = pltpu.SemaphoreType.DMA
    regular = pltpu.SemaphoreType.REGULAR
    any_spec = pl.BlockSpec(memory_space=pltpu.HBM)
    vmem = pl.BlockSpec(memory_space=pltpu.VMEM)
    smem = pl.BlockSpec(memory_space=pltpu.SMEM)
    part, res, own = pl.pallas_call(
        functools.partial(kernel, cx, cy, nz, nrow),
        out_shape=(
            pltpu.VMEM((3 * cells, nz), f32),
            pltpu.VMEM((9, CAP, 3 * nz), f32),
            pltpu.SMEM((9, 1, 128), jnp.int32),
        ),
        in_specs=[any_spec] * 9,
        out_specs=(vmem, vmem, smem),
        scratch_shapes=[
            pltpu.VMEM((4 * cells, nz), f32),
            pltpu.VMEM((3 * cells, nz), f32),
            pltpu.VMEM((cells, nz), f32),
            pltpu.VMEM((kinds, nz), f32),
            pltpu.VMEM((3, nrow), jnp.int32),
            pltpu.SMEM((1,), jnp.int32),
            pltpu.VMEM((nrow,), jnp.int32),
            pltpu.VMEM((9, 1, 128), jnp.int32),
            pltpu.SMEM((9, 1, 128), jnp.int32),
            pltpu.VMEM((9, ROWS, 2 * nz), f32),
            pltpu.VMEM((9, ROWS, 2 * nz), f32),
            pltpu.VMEM((9, ROWS, 2 * nz), f32),
            pltpu.VMEM((9, ROWS, nz), f32),
            pltpu.VMEM((9, CAP, 3 * nz), f32),
            pltpu.VMEM((8, CAP, 3 * nz), f32),
            pltpu.VMEM((9, CAP, nz), f32),
            pltpu.VMEM((2, 5, cy, nz), f32),
            pltpu.VMEM((4, 5, cx, nz), f32),
            dma((5,)), dma((5,)), dma, dma((2,)), dma((2,)),
            pltpu.VMEM((3, cy, nz), f32),
            pltpu.VMEM((6, 1, 128), jnp.int32),
            pltpu.VMEM((6, ROWS, 2 * nz), f32),
            dma((4,)), dma((4,)), regular((2,)), regular, regular,
        ],
        compiler_params=pltpu.CompilerParams(
            collective_id=0, has_side_effects=True, vmem_limit_bytes=60000000
        ),
    )(
        pressure.reshape(cells, nz),
        depth.reshape(cells, nz),
        saturation.reshape(2 * cells, nz),
        permeability.reshape(3 * cells, nz),
        pore_volume.reshape(cells, nz),
        pairs.T,
        kind,
        count,
        table,
    )
    _, _, out = pl.pallas_call(
        functools.partial(finish, cells, nz),
        out_shape=(
            pltpu.VMEM((3 * cells, nz), f32),
            pltpu.VMEM((9, CAP, 3 * nz), f32),
            jax.ShapeDtypeStruct((3 * cells, nz), f32),
        ),
        in_specs=[vmem, vmem, smem],
        out_specs=(vmem, vmem, any_spec),
        scratch_shapes=[dma],
        input_output_aliases={0: 0, 1: 1},
    )(part, res, own)
    return out.reshape(3, cx, cy, nz)


def solution(mesh):
    cell = P("gx", "gy", None)
    cells = P(None, "gx", "gy", None)
    both = ("gx", "gy")
    return jax.shard_map(
        body,
        mesh=mesh,
        in_specs=(cell, cell, cells, cells, cell, P(both, None), P(both), P(both), P()),
        out_specs=cells,
        check_vma=False,
    )
```

```python
import functools

import jax
import jax.numpy as jnp
from jax import lax
from jax.experimental import pallas as pl
from jax.experimental.pallas import tpu as pltpu
from jax.sharding import PartitionSpec as P

CAP = 4
ROWS = 2 * CAP
VISCOSITY = (0.5, 1.0, 0.25)
DENSITY = (1.0, 0.8, 0.25)
STEP = 0.2
MESH = pl.DeviceIdType.MESH
NEAR = [(dx, dy) for dx in (-1, 0, 1) for dy in ((-1, 1, 0) if dx == 0 else (-1, 0, 1))]
HOME = 5
OTHERS = [n for n in range(9) if n != HOME]
PIECES = 24


def mobility(w, o):
    g = 1.0 - w - o
    return (w * w * (1.0 / VISCOSITY[0]), o * o, g * g * (1.0 / VISCOSITY[2]))


def harmonic(a, b):
    return 2.0 * a * b / (a + b)


def flux(dp, dd, low, high, trans):
    flows = []
    for f in range(3):
        drive = dp - DENSITY[f] * dd if DENSITY[f] != 1.0 else dp - dd
        flows.append(trans * jnp.where(drive > 0.0, low[f], high[f]) * drive)
    return flows


def edge_flux(low, high):
    return flux(
        low[0] - high[0],
        low[1] - high[1],
        mobility(low[2], low[3]),
        mobility(high[2], high[3]),
        harmonic(low[4], high[4]),
    )


def kernel(
    cx, cy, nz, nrow,
    p_hbm, d_hbm, s_hbm, k_hbm, v_hbm, pairs_hbm, kind_hbm, count_hbm, table_hbm,
    out, res, own_s,
    cell, k, v, table, pairs_v, count_s, kindrow,
    idx_send, idx_s, send, recv, loc, tloc, back, ret, scl,
    xhalo, yhalo,
    ir_sem, fr_sem, br_sem, xr_sem, yr_sem,
    between, via_i, via_f, vi_sem, vf_sem, go_sem, here_sem, near_sem,
):
    def arrived(ref, sem):
        pltpu.make_async_copy(ref, ref, sem).wait()

    def seat(n):
        return n - 1 if isinstance(n, int) and n > HOME else n

    def work(load_sem, own_sem, out_sem, ws_sem, xs_sem, ys_sem):
        nx = lax.axis_size("gx")
        ny = lax.axis_size("gy")
        ix = lax.axis_index("gx")
        iy = lax.axis_index("gy")
        cells = cx * cy
        p, d, s = (cell.at[pl.ds(i * cells, (1, 1, 2)[i] * cells)] for i in range(3))

        def device(dx, dy):
            return (lax.rem(ix + dx + nx, nx), lax.rem(iy + dy + ny, ny))

        def remote(src, dst, ss, rs, dev):
            return pltpu.make_async_remote_copy(
                src_ref=src, dst_ref=dst, send_sem=ss, recv_sem=rs, device_id=dev, device_id_type=MESH
            )

        def signal(sem, dev):
            pl.semaphore_signal(sem, inc=1, device_id=dev, device_id_type=MESH)

        def wrap(y):
            return lax.rem(y + 2 * ny, ny)

        first, last = ix == 0, ix == nx - 1
        y_odd = lax.rem(iy, 2)
        relays = (ix == 1) & (y_odd == 1)
        barrier = pltpu.get_barrier_semaphore()
        for n in OTHERS:
            dx, dy = NEAR[n]
            if dx == 1:
                @pl.when(ix < nx - 2)
                def _():
                    signal(barrier, device(dx, dy))
            elif dx == 0:
                @pl.when(~first & ~last)
                def _():
                    signal(barrier, device(dx, dy))
            else:
                @pl.when((ix > 1) | relays)
                def _():
                    signal(barrier, device(dx, dy))

        @pl.when(first & (y_odd == 1))
        def _():
            signal(barrier, (1, wrap(iy + 2)))

        @pl.when(relays)
        def _():
            signal(barrier, (nx - 1, wrap(iy - 1)))
            signal(barrier, (nx - 1, iy))
            signal(barrier, (0, wrap(iy - 2)))

        @pl.when(last)
        def _():
            pl.semaphore_wait(barrier, 1)
            signal(go_sem.at[y_odd], (1, iy + 1 - y_odd))

        loads = [
            pltpu.make_async_copy(src, dst, load_sem.at[i])
            for i, src, dst in (
                (0, pairs_hbm, pairs_v),
                (1, kind_hbm, kindrow),
                (2, count_hbm, count_s),
                (3, p_hbm, p),
                (3, d_hbm, d),
                (3, s_hbm, s),
                (4, k_hbm, k),
                (5, v_hbm, v),
                (6, table_hbm, table),
            )
        ]
        for c in loads:
            c.start()

        for c in loads[:3]:
            c.wait()
        lane_of_row = lax.broadcasted_iota(jnp.int32, (nrow, nrow), 1)
        sub_of_row = lax.broadcasted_iota(jnp.int32, (nrow, nrow), 0)
        eye = lane_of_row == sub_of_row
        pv = pairs_v[...]
        tgt_row = pv[1:2, :]

        def to_sublanes(row):
            return jnp.sum(jnp.where(eye, row, 0), axis=1, keepdims=True)

        src_col = to_sublanes(pv[0:1, :])
        tgt_col = to_sublanes(tgt_row)
        land_col = to_sublanes(pv[2:3, :])
        kind_col = to_sublanes(kindrow[...].reshape(1, nrow))
        rank_col = jnp.sum(
            ((tgt_col == tgt_row) & (lane_of_row < sub_of_row)).astype(jnp.int32), axis=1, keepdims=True
        )
        live_col = (lax.broadcasted_iota(jnp.int32, (nrow, 1), 0) < count_s[0]).astype(jnp.int32)
        code_col = jnp.zeros_like(tgt_col)
        for n in range(9):
            hx, hy = device(*NEAR[n])
            code_col = jnp.where(tgt_col == hx * ny + hy, n, code_col)
        lanes = lax.broadcasted_iota(jnp.int32, (nrow, 128), 1)
        message = (
            jnp.where(lanes == rank_col, land_col, 0)
            + jnp.where(lanes == CAP + rank_col, kind_col, 0)
            + jnp.where(lanes == 2 * CAP + rank_col, live_col, 0)
            + jnp.where(lanes == 3 * CAP + rank_col, src_col, 0)
        )
        for n in range(9):
            idx_send[n] = jnp.sum(jnp.where(code_col == n, message, 0), axis=0, keepdims=True)

        own_copy = pltpu.make_async_copy(idx_send, own_s, own_sem)
        own_copy.start()
        arrived(cell, load_sem.at[3])
        own_copy.wait()
        for n in range(9):
            dst = recv if n == HOME else send
            for r in range(CAP):
                col = own_s[n, 0, 3 * CAP + r]
                dst[n, r : r + 1, :nz] = p[pl.ds(col, 1), :]
                dst[n, CAP + r : CAP + r + 1, :nz] = d[pl.ds(col, 1), :]
                dst[n, r : r + 1, nz:] = s[pl.ds(col, 1), :]
                dst[n, CAP + r : CAP + r + 1, nz:] = s[pl.ds(cells + col, 1), :]

        odd = lax.rem(ix, 2)
        away = 2 * odd - 1

        def place(dx, dy):
            if isinstance(dx, int) and dx == 0:
                return NEAR.index((0, dy))
            return 3 * (dx + 1) + dy + 1

        def ask(dx, dy):
            n = place(dx, dy)
            dev = device(dx, dy)
            slot = inbox(dx, dy)
            remote(idx_send.at[n], idx_s.at[n], out_sem, ir_sem.at[slot], dev).start()
            remote(send.at[n], recv.at[n], out_sem, fr_sem.at[slot], dev).start()

        def inbox(dx, dy):
            if isinstance(dx, int):
                return dy + 1 if dx < 0 else 3 + dx
            return jnp.where(dx < 0, dy + 1, 3 + dx)

        def relay_slot(j, off):
            if isinstance(off, int):
                return (0, 1 + j, 3 + j, 5)[off + 2]
            return jnp.where(off == -2, 0, jnp.where(off == -1, 1 + j, jnp.where(off == 0, 3 + j, 5)))

        def far_asks():
            for dy in (-1, 1, 0):
                ask(away, dy)

        def near_asks():
            for dy in (-1, 1, 0):
                ask(-away, dy)
            for dy in (-1, 1):
                ask(0, dy)

        @pl.when(first)
        def _():
            pl.semaphore_wait(barrier, 2)
            for dy in (y_odd, 1 - 2 * y_odd, y_odd - 1):
                ty = wrap(iy + dy)
                t_odd = lax.rem(ty, 2)
                off = t_odd - 1 - dy
                slot = relay_slot(t_odd, off)
                via = (1, ty + 1 - t_odd)
                remote(idx_send.at[dy + 1], via_i.at[slot], out_sem, vi_sem.at[off + 2], via).start()
                remote(send.at[dy + 1], via_f.at[slot], out_sem, vf_sem.at[off + 2], via).start()

        @pl.when(~first)
        def _():
            @pl.when(~last)
            def _():
                pl.semaphore_wait(barrier, 8 + relays.astype(jnp.int32))

            @pl.when(relays)
            def _():
                signal(barrier, (nx - 1, wrap(iy - 1)))
                signal(barrier, (nx - 1, iy))
                for off in (-2, -1, 0, 1):
                    signal(near_sem, (0, wrap(iy + off)))

            @pl.when(ix == nx - 2)
            def _():
                for dy in (-1, 0, 1):
                    signal(here_sem, device(1, dy))

            @pl.when(last)
            def _():
                pl.semaphore_wait(barrier, 1)
                for dy in (-1, 0, 1):
                    signal(here_sem, device(1, dy))
                pl.semaphore_wait(here_sem, 3)

            @pl.when(ix != 2)
            def _():
                far_asks()

        @pl.when(~first & (ix != 2))
        def _():
            near_asks()

        for c in loads[6:]:
            c.wait()
        xparts = [(p, 0), (d, 0), (s, 0), (s, cells), (k, 0)]
        yparts = [(p, 0), (d, 0), (s, 0), (s, cx), (k, cx)]

        def xcopy(side, f):
            ref, base = xparts[f]
            at = base + (0 if side == 0 else cells - cy)
            return remote(
                ref.at[pl.ds(at, cy), :], xhalo.at[1 - side, f], xs_sem.at[side], xr_sem.at[1 - side],
                device(-1 if side == 0 else 1, 0),
            )

        for f in range(5):
            ref, base = yparts[f]
            base = base * cy if f >= 3 else base
            for side in range(2):
                off = base + (0 if side == 0 else cy - 1)
                yhalo[2 + side, f] = ref[pl.ds(off, cx, stride=cy), :]

        def ycopy(side):
            return remote(
                yhalo.at[2 + side], yhalo.at[1 - side], ys_sem.at[side], yr_sem.at[1 - side],
                device(0, -1 if side == 0 else 1),
            )

        zmask = lax.broadcasted_iota(jnp.int32, (cy, nz), 1) < nz - 1
        ymask = lax.broadcasted_iota(jnp.int32, (cy, nz), 0) < cy - 1

        def slab(a, carry):
            base = pl.multiple_of(a * cy, cy)
            after = pl.multiple_of(jnp.minimum(a + 1, cx - 1) * cy, cy)

            def at(ref, off):
                return ref[pl.ds(off, cy), :]

            p0, d0 = at(p, base), at(d, base)
            w0, o0 = at(s, base), at(s, cells + base)
            m0 = mobility(w0, o0)
            m1 = mobility(at(s, after), at(s, cells + after))
            tx = jnp.where(a < cx - 1, harmonic(at(k, base), at(k, after)), 0.0)
            fx = flux(p0 - at(p, after), d0 - at(d, after), m0, m1, tx)
            net = [fx[f] - carry[f] for f in range(3)]
            for axis, size, mask, offset in ((0, cy, ymask, cells), (1, nz, zmask, 2 * cells)):
                def up(x):
                    return pltpu.roll(x, size - 1, axis)

                kk = at(k, offset + base)
                t = jnp.where(mask, harmonic(kk, up(kk)), 0.0)
                fl = flux(p0 - up(p0), d0 - up(d0), m0, [up(m) for m in m0], t)
                net = [net[f] + (fl[f] - pltpu.roll(fl[f], 1, axis)) for f in range(3)]
            scale = STEP / at(v, base)
            v[pl.ds(base, cy), :] = scale
            now = (w0, o0, 1.0 - w0 - o0)
            for f in range(3):
                out[pl.ds(f * cells + base, cy), :] = now[f] - scale * net[f]
            return tuple(fx)

        zero = jnp.zeros((cy, nz), jnp.float32)
        quarter = cx // 4

        def march(start, stop):
            before = tuple(between[f] for f in range(3)) if start else (zero, zero, zero)
            edge = lax.fori_loop(start, stop, slab, before, unroll=2)
            if stop < cx:
                for f in range(3):
                    between[f] = edge[f]

        march(0, quarter)

        @pl.when(ix == 2)
        def _():
            far_asks()

        @pl.when(first)
        def _():
            pl.semaphore_wait(near_sem, 2)

        @pl.when(first | (ix == 2))
        def _():
            near_asks()

        def take(off):
            start, many = ((0, 1), (1, 2), (3, 2), (5, 1))[off + 2]
            arrived(via_i.at[pl.ds(start, many)], vi_sem.at[off + 2])
            arrived(via_f.at[pl.ds(start, many)], vf_sem.at[off + 2])

        def onward(j, off):
            dy = j - 1 - off
            slot, dev = relay_slot(j, off), (nx - 1, wrap(iy - 1 + j))
            remote(via_i.at[slot], idx_s.at[dy + 1], ws_sem, ir_sem.at[dy + 1], dev).start()
            remote(via_f.at[slot], recv.at[dy + 1], ws_sem, fr_sem.at[dy + 1], dev).start()

        def pass_on(plan):
            for step in plan:
                if step in ("even", "odd"):
                    pl.semaphore_wait(go_sem.at[int(step == "odd")], 1)
                elif isinstance(step, int):
                    take(step)
                else:
                    onward(*step)

        @pl.when(relays & (iy == 1))
        def _():
            pass_on(["odd", "even", 0, (0, 0), (1, 0), -1, (0, -1), (1, -1), -2, (0, -2), 1, (1, 1)])

        @pl.when(relays & (iy != 1))
        def _():
            pass_on(["even", -2, (0, -2), "odd", 1, (1, 1), 0, (0, 0), (1, 0), -1, (0, -1), (1, -1)])

        march(quarter, 2 * quarter)
        has = ((ix > 0, ix < nx - 1), (iy > 0, iy < ny - 1))
        for side in range(2):
            @pl.when(has[0][side])
            def _():
                for f in range(5):
                    xcopy(side, f).start()

            @pl.when(has[1][side])
            def _():
                ycopy(side).start()

        @pl.when(~last)
        def _():
            march(2 * quarter, cx)

        def answer(n, ints):
            for r in range(CAP):
                land = ints[n, 0, r]
                kd = ints[n, 0, CAP + r]
                live = ints[n, 0, 2 * CAP + r].astype(jnp.float32)
                loc[n, r : r + 1, :nz] = p[pl.ds(land, 1), :]
                loc[n, CAP + r : CAP + r + 1, :nz] = d[pl.ds(land, 1), :]
                loc[n, r : r + 1, nz:] = s[pl.ds(land, 1), :]
                loc[n, CAP + r : CAP + r + 1, nz:] = s[pl.ds(cells + land, 1), :]
                tloc[n, r : r + 1, :] = table[pl.ds(kd, 1), :] * live

        def flows_of(start, many):
            rows = pl.ds(start, many)
            far, here = recv[rows], loc[rows]

            def second(x):
                return pltpu.roll(x, CAP, 1)

            gap = far[:, :, :nz] - here[:, :, :nz]
            fl = flux(
                gap,
                second(gap),
                mobility(far[:, :, nz:], second(far[:, :, nz:])),
                mobility(here[:, :, nz:], second(here[:, :, nz:])),
                tloc[rows],
            )
            for f in range(3):
                back[rows, :, f * nz : (f + 1) * nz] = fl[f][:, :CAP]

        def reply(dx, dy):
            n = place(dx, dy)
            return remote(back.at[n], ret.at[seat(n)], out_sem, br_sem, device(-dx, -dy))

        def landed(buf, sem, dx):
            start = 3 * (dx + 1)
            if dx < 0:
                for i in range(3):
                    arrived(buf.at[i], sem.at[i])
            else:
                arrived(buf.at[pl.ds(start, 2 + dx)], sem.at[3 + dx])

        def serve(dx):
            start = 3 * (dx + 1)
            landed(idx_s, ir_sem, dx)
            for i in range(3):
                answer(start + i, own_s if start + i == HOME else idx_s)
            landed(recv, fr_sem, dx)
            flows_of(start, 3)
            if dx == 1:
                @pl.when(first)
                def _():
                    pl.semaphore_wait(here_sem, 3)

            for dy in (-1, 1, 0):
                if dx or dy:
                    reply(dx, dy).start()

        @pl.when(last)
        def _():
            side = jnp.where((iy == 0) | (iy == ny - 1), -1, 1)
            for dy in (side, 0, -side):
                n = dy + 1
                arrived(idx_s.at[n], ir_sem.at[n])
                answer(n, idx_s)
                arrived(recv.at[n], fr_sem.at[n])
                flows_of(n, 1)
                reply(-1, dy).start()

        serve(0)

        @pl.when(odd == 1)
        def _():
            serve(1)

        @pl.when(~last)
        def _():
            serve(-1)

        @pl.when(odd == 0)
        def _():
            serve(1)

        @pl.when(last)
        def _():
            march(2 * quarter, cx)

        for side in range(2):
            @pl.when(has[0][side])
            def _():
                arrived(xhalo.at[side], xs_sem.at[side])
                arrived(xhalo.at[side], xr_sem.at[side])
                at = 0 if side == 0 else cells - cy
                mine = [ref[pl.ds(base + at, cy), :] for ref, base in xparts]
                near = [xhalo[side, f] for f in range(5)]
                low, high = (near, mine) if side == 0 else (mine, near)
                fl = edge_flux(low, high)
                scale = v[pl.ds(at, cy), :]
                for f in range(3):
                    rows = pl.ds(f * cells + at, cy)
                    out[rows, :] = out[rows, :] + (scale * fl[f] if side == 0 else -scale * fl[f])

        for side in range(2):
            @pl.when(has[1][side])
            def _():
                ycopy(side).wait_send()
                ycopy(1 - side).wait_recv()
                at = 0 if side == 0 else cy - 1
                mine = [yhalo[2 + side, f] for f in range(5)]
                near = [yhalo[side, f] for f in range(5)]
                low, high = (near, mine) if side == 0 else (mine, near)
                fl = edge_flux(low, high)
                scale = v[pl.ds(at, cx, stride=cy), :]
                for f in range(3):
                    rows = pl.ds(f * cells + at, cx, stride=cy)
                    out[rows, :] = out[rows, :] + (scale * fl[f] if side == 0 else -scale * fl[f])

        lane1 = lax.broadcasted_iota(jnp.int32, (1, 128), 1)
        slots = 10 * CAP
        spot = jnp.full((1, 128), -1, jnp.int32)
        for n in range(9):
            for r in range(CAP):
                spot = jnp.where(lane1 == n * CAP + r, (own_s if n == HOME else idx_s)[n, 0, r], spot)
        for r in range(CAP):
            spot = jnp.where(lane1 == 9 * CAP + r, own_s[HOME, 0, 3 * CAP + r], spot)
        spot = jnp.where(lane1 < slots, spot, 0)
        spot = spot + pltpu.roll(spot, slots, 1) + pltpu.roll(spot, 2 * slots, 1)
        flows = jnp.concatenate([-back[n] for n in range(9)] + [back[HOME]], axis=0)
        hi = flows.astype(jnp.bfloat16).astype(jnp.float32)
        rest = flows - hi
        mid = rest.astype(jnp.bfloat16).astype(jnp.float32)
        pad = jnp.zeros((128 - 3 * slots, 3 * nz), jnp.float32)
        parts = jnp.concatenate([hi, mid, rest - mid, pad], axis=0).astype(jnp.bfloat16)
        step = 8 * cy
        for c in range(cells // step):
            ids = lax.broadcasted_iota(jnp.int32, (step, 128), 0) + c * step
            hot = (ids == spot).astype(jnp.float32).astype(jnp.bfloat16)
            add = jnp.dot(hot, parts, preferred_element_type=jnp.float32)
            scale = v[c * step : (c + 1) * step, :]
            for f in range(3):
                at = pl.ds(f * cells + c * step, step)
                out[at, :] = out[at, :] - scale * add[:, f * nz : (f + 1) * nz]

        for n in OTHERS:
            for r in range(CAP):
                scl[n, r : r + 1, :] = v[pl.ds(own_s[n, 0, 3 * CAP + r], 1), :]
        @pl.when(relays)
        def _():
            arrived(cell.at[pl.ds(0, 6 * (1 + 2 * ROWS))], ws_sem)

        arrived(cell.at[pl.ds(0, 8 * (1 + 2 * ROWS + 3 * CAP))], out_sem)
    dma = pltpu.SemaphoreType.DMA
    pl.run_scoped(work, dma((7,)), dma, dma, dma, dma((2,)), dma((2,)))
    arrived(ret, br_sem)
    for n in OTHERS:
        for f in range(3):
            res[n, :, f * nz : (f + 1) * nz] = ret[seat(n), :, f * nz : (f + 1) * nz] * scl[n]


def finish(cells, nz, part, res_in, own_s, held, res, final, sem):
    for n in OTHERS:
        for r in range(CAP):
            col = own_s[n, 0, 3 * CAP + r]
            for f in range(3):
                row = pl.ds(f * cells + col, 1)
                held[row, :] = held[row, :] - res[n, r : r + 1, f * nz : (f + 1) * nz]
    size = 3 * cells // PIECES
    for i in range(PIECES):
        rows = pl.ds(i * size, size)
        pltpu.make_async_copy(held.at[rows], final.at[rows], sem).start()
    pltpu.make_async_copy(held, final, sem).wait()


def body(pressure, depth, saturation, permeability, pore_volume, pairs, kind, count, table):
    cx, cy, nz = pressure.shape
    nrow = pairs.shape[0]
    kinds = table.shape[0]
    cells = cx * cy
    f32 = jnp.float32
    dma = pltpu.SemaphoreType.DMA
    regular = pltpu.SemaphoreType.REGULAR
    any_spec = pl.BlockSpec(memory_space=pltpu.HBM)
    vmem = pl.BlockSpec(memory_space=pltpu.VMEM)
    smem = pl.BlockSpec(memory_space=pltpu.SMEM)
    part, res, own = pl.pallas_call(
        functools.partial(kernel, cx, cy, nz, nrow),
        out_shape=(
            pltpu.VMEM((3 * cells, nz), f32),
            pltpu.VMEM((9, CAP, 3 * nz), f32),
            pltpu.SMEM((9, 1, 128), jnp.int32),
        ),
        in_specs=[any_spec] * 9,
        out_specs=(vmem, vmem, smem),
        scratch_shapes=[
            pltpu.VMEM((4 * cells, nz), f32),
            pltpu.VMEM((3 * cells, nz), f32),
            pltpu.VMEM((cells, nz), f32),
            pltpu.VMEM((kinds, nz), f32),
            pltpu.VMEM((3, nrow), jnp.int32),
            pltpu.SMEM((1,), jnp.int32),
            pltpu.VMEM((nrow,), jnp.int32),
            pltpu.VMEM((9, 1, 128), jnp.int32),
            pltpu.SMEM((9, 1, 128), jnp.int32),
            pltpu.VMEM((9, ROWS, 2 * nz), f32),
            pltpu.VMEM((9, ROWS, 2 * nz), f32),
            pltpu.VMEM((9, ROWS, 2 * nz), f32),
            pltpu.VMEM((9, ROWS, nz), f32),
            pltpu.VMEM((9, CAP, 3 * nz), f32),
            pltpu.VMEM((8, CAP, 3 * nz), f32),
            pltpu.VMEM((9, CAP, nz), f32),
            pltpu.VMEM((2, 5, cy, nz), f32),
            pltpu.VMEM((4, 5, cx, nz), f32),
            dma((5,)), dma((5,)), dma, dma((2,)), dma((2,)),
            pltpu.VMEM((3, cy, nz), f32),
            pltpu.VMEM((6, 1, 128), jnp.int32),
            pltpu.VMEM((6, ROWS, 2 * nz), f32),
            dma((4,)), dma((4,)), regular((2,)), regular, regular,
        ],
        compiler_params=pltpu.CompilerParams(
            collective_id=0, has_side_effects=True, vmem_limit_bytes=60000000
        ),
    )(
        pressure.reshape(cells, nz),
        depth.reshape(cells, nz),
        saturation.reshape(2 * cells, nz),
        permeability.reshape(3 * cells, nz),
        pore_volume.reshape(cells, nz),
        pairs.T,
        kind,
        count,
        table,
    )
    _, _, out = pl.pallas_call(
        functools.partial(finish, cells, nz),
        out_shape=(
            pltpu.VMEM((3 * cells, nz), f32),
            pltpu.VMEM((9, CAP, 3 * nz), f32),
            jax.ShapeDtypeStruct((3 * cells, nz), f32),
        ),
        in_specs=[vmem, vmem, smem],
        out_specs=(vmem, vmem, any_spec),
        scratch_shapes=[dma],
        input_output_aliases={0: 0, 1: 1},
    )(part, res, own)
    return out.reshape(3, cx, cy, nz)


def solution(mesh):
    cell = P("gx", "gy", None)
    cells = P(None, "gx", "gy", None)
    both = ("gx", "gy")
    return jax.shard_map(
        body,
        mesh=mesh,
        in_specs=(cell, cell, cells, cells, cell, P(both, None), P(both), P(both), P()),
        out_specs=cells,
        check_vma=False,
    )
```
